16 devices in a mesh: sample: 2 (over y, z), tok: 8 (over x, core).
Axes of the slice: x: 4, y: 2, z: 1, core: 2. Of those that a mesh axis runs over, the one named last changes fastest.
The devices are a block of a 4x4x8 slice.
Arguments:
- s_trunk: bfloat16 [1024, 128], P('tok')
- s_inputs: bfloat16 [1024, 128], P('tok')
- z_trunk: bfloat16 [1024, 1024, 16], P('tok')
- x_noise: float32 [2048, 3], P(('sample', 'tok')), parts along dimension 0
- step_noise: float32 [3, 2048, 3], P(None, ('sample', 'tok')), parts along dimension 1
- sigmas: float32 [4], replicated
- relpos_table: bfloat16 [65, 16], replicated
- w_pair_in: bfloat16 [32, 16], replicated
- w_z_up: bfloat16 [2, 16, 64], replicated
- w_z_down: bfloat16 [2, 32, 16], replicated
- w_pair_bias: bfloat16 [2, 16, 4], replicated
- w_single: bfloat16 [256, 128], replicated
- fourier_w: float32 [256], replicated
- fourier_b: float32 [256], replicated
- w_fourier: bfloat16 [256, 128], replicated
- w_s_up: bfloat16 [2, 128, 512], replicated
- w_s_down: bfloat16 [2, 256, 128], replicated
- w_in: float32 [3, 128], replicated
- w_s_tok: bfloat16 [128, 128], replicated
- w_cond: bfloat16 [2, 128, 768], replicated
- gate_bias: float32 [2, 2, 128], replicated
- w_qkvg: bfloat16 [2, 128, 512], replicated
- w_attn_out: bfloat16 [2, 128, 128], replicated
- w_up: bfloat16 [2, 128, 512], replicated
- w_down: bfloat16 [2, 256, 128], replicated
- w_out: bfloat16 [128, 3], replicated
Outputs:
- output: float32 [2048, 3], P(('sample', 'tok')), parts along dimension 0
There are 2 independent parts. The reference program is written for one: setup_inputs(seed, part) draws one part's arguments, and reference() takes and returns one part's arrays. A program takes and returns all parts, laid end to end along the dimension named above; an argument that names none is the same for every part.
All inputs are finite; a program needn't handle non-finite values.
Results may differ from the reference program's by a relative error of at most 0.00403962.
Values are sent between devices in bfloat16 or wider.
A program may use at most 768 MiB of HBM per device.

```python
import math
import jax
import jax.numpy as jnp
from jax import lax

N_TOKENS = 1024
N_VALID = 992
C_TOKEN = 128
C_S = 128
C_Z = 16
HEADS = 4
BLOCKS = 2
STEPS = 3
FOURIER = 256
REL_BINS = 65
ROW_BLOCK = 8
HEAD_DIM = C_TOKEN // HEADS
REL_CLIP = (REL_BINS - 1) // 2
SIGMA_DATA = 16.0
GAMMA = 0.8
NOISE_SCALE = 1.003
STEP_SCALE = 1.5
MASK_VALUE = -1e9


def normal_weight(rng_key, shape_dims, fan_in, weight_gain=1.0):
    raw_draw = jax.random.normal(rng_key, shape_dims, jnp.float32)
    return (raw_draw * (weight_gain / math.sqrt(fan_in))).astype(jnp.bfloat16)


def setup_inputs(seed: int = 0, part: int = 0) -> dict:
    key_list = jax.random.split(jax.random.key(seed), 24)
    part_keys = jax.random.split(jax.random.fold_in(jax.random.key(seed + 1), part), 2)
    level_idx = jnp.arange(STEPS + 1).astype(jnp.float32)
    jitter = jax.random.uniform(key_list[5], (STEPS + 1,), jnp.float32, -1.0, 1.0)
    sigmas = jnp.exp(math.log(160.0) * (1.0 - level_idx / STEPS) + 0.2 * jitter)
    return {
        "s_trunk": jax.random.normal(key_list[0], (N_TOKENS, C_S), jnp.float32).astype(jnp.bfloat16),
        "s_inputs": jax.random.normal(key_list[1], (N_TOKENS, C_S), jnp.float32).astype(jnp.bfloat16),
        "z_trunk": jax.random.normal(key_list[2], (N_TOKENS, N_TOKENS, C_Z), jnp.float32).astype(jnp.bfloat16),
        "x_noise": jax.random.normal(part_keys[0], (N_TOKENS, 3), jnp.float32),
        "step_noise": jax.random.normal(part_keys[1], (STEPS, N_TOKENS, 3), jnp.float32),
        "sigmas": sigmas,
        "relpos_table": jax.random.normal(key_list[6], (REL_BINS, C_Z), jnp.float32).astype(jnp.bfloat16),
        "w_pair_in": normal_weight(key_list[7], (2 * C_Z, C_Z), 2 * C_Z),
        "w_z_up": normal_weight(key_list[8], (2, C_Z, 4 * C_Z), C_Z),
        "w_z_down": normal_weight(key_list[9], (2, 2 * C_Z, C_Z), 2 * C_Z),
        "w_pair_bias": normal_weight(key_list[10], (BLOCKS, C_Z, HEADS), C_Z, 3.0),
        "w_single": normal_weight(key_list[11], (2 * C_S, C_S), 2 * C_S),
        "fourier_w": jax.random.normal(key_list[12], (FOURIER,), jnp.float32),
        "fourier_b": jax.random.uniform(key_list[13], (FOURIER,), jnp.float32),
        "w_fourier": normal_weight(key_list[14], (FOURIER, C_S), FOURIER),
        "w_s_up": normal_weight(key_list[15], (2, C_S, 4 * C_S), C_S),
        "w_s_down": normal_weight(key_list[16], (2, 2 * C_S, C_S), 2 * C_S),
        "w_in": jax.random.normal(key_list[17], (3, C_TOKEN), jnp.float32) / math.sqrt(3.0),
        "w_s_tok": normal_weight(key_list[18], (C_S, C_TOKEN), C_S),
        "w_cond": normal_weight(key_list[19], (BLOCKS, C_S, 6 * C_TOKEN), C_S),
        "gate_bias": -1.0 + jax.random.normal(key_list[20], (BLOCKS, 2, C_TOKEN), jnp.float32),
        "w_qkvg": normal_weight(key_list[21], (BLOCKS, C_TOKEN, 4 * C_TOKEN), C_TOKEN),
        "w_attn_out": normal_weight(key_list[22], (BLOCKS, C_TOKEN, C_TOKEN), C_TOKEN),
        "w_up": normal_weight(key_list[23], (BLOCKS, C_TOKEN, 4 * C_TOKEN), C_TOKEN),
        "w_down": normal_weight(key_list[3], (BLOCKS, 2 * C_TOKEN, C_TOKEN), 2 * C_TOKEN),
        "w_out": normal_weight(key_list[4], (C_TOKEN, 3), C_TOKEN),
    }


def layer_norm(values):
    values = values.astype(jnp.float32)
    centered = values - jnp.mean(values, axis=-1, keepdims=True)
    variance = jnp.mean(centered * centered, axis=-1, keepdims=True)
    return centered * lax.rsqrt(variance + 1e-5)


def transition(values, w_up_one, w_down_one):
    hidden = jnp.dot(layer_norm(values).astype(jnp.bfloat16), w_up_one, preferred_element_type=jnp.float32)
    half_width = hidden.shape[-1] // 2
    gated_act = (jax.nn.silu(hidden[:, :half_width]) * hidden[:, half_width:]).astype(jnp.bfloat16)
    return values + jnp.dot(gated_act, w_down_one, preferred_element_type=jnp.float32)


def pair_bias(z_trunk, relpos_table, w_pair_in, w_z_up, w_z_down, w_pair_bias):
    col_ids = jnp.arange(N_TOKENS)
    bias_weight = jnp.transpose(w_pair_bias, (1, 0, 2)).reshape(C_Z, BLOCKS * HEADS)
    z_groups = z_trunk.reshape(N_TOKENS // ROW_BLOCK, ROW_BLOCK, N_TOKENS, C_Z)
    row_groups = jnp.arange(N_TOKENS).reshape(N_TOKENS // ROW_BLOCK, ROW_BLOCK)

    def one_group(group_in):
        z_group, row_ids = group_in
        bin_index = jnp.clip(row_ids[:, None] - col_ids[None, :] + REL_CLIP, 0, REL_BINS - 1)
        rel_feat = relpos_table[bin_index]
        pair_in = layer_norm(jnp.concatenate([z_group, rel_feat], axis=-1)).astype(jnp.bfloat16)
        pair_cond = jnp.dot(pair_in.reshape(-1, 2 * C_Z), w_pair_in, preferred_element_type=jnp.float32)
        for layer_idx in range(w_z_up.shape[0]):
            pair_cond = transition(pair_cond, w_z_up[layer_idx], w_z_down[layer_idx])
        bias_flat = jnp.dot(layer_norm(pair_cond).astype(jnp.bfloat16), bias_weight, preferred_element_type=jnp.float32)
        return bias_flat.astype(jnp.bfloat16).reshape(ROW_BLOCK, N_TOKENS, BLOCKS, HEADS)

    groups = lax.map(one_group, (z_groups, row_groups))
    return jnp.transpose(groups.reshape(N_TOKENS, N_TOKENS, BLOCKS, HEADS), (2, 3, 0, 1))


def single_cond(s_base, t_hat, fourier_w, fourier_b, w_fourier, w_s_up, w_s_down):
    noise_level = 0.25 * jnp.log(t_hat / SIGMA_DATA)
    fourier_feat = jnp.cos(2.0 * math.pi * (noise_level * fourier_w + fourier_b))
    fourier_emb = jnp.dot(layer_norm(fourier_feat[None, :]).astype(jnp.bfloat16), w_fourier, preferred_element_type=jnp.float32)
    single = s_base + fourier_emb
    for layer_idx in range(w_s_up.shape[0]):
        single = transition(single, w_s_up[layer_idx], w_s_down[layer_idx])
    return layer_norm(single).astype(jnp.bfloat16)


def reference(s_trunk, s_inputs, z_trunk, x_noise, step_noise, sigmas, relpos_table, w_pair_in, w_z_up, w_z_down, w_pair_bias, w_single, fourier_w, fourier_b, w_fourier, w_s_up, w_s_down, w_in, w_s_tok, w_cond, gate_bias, w_qkvg, w_attn_out, w_up, w_down, w_out):
    bias_all = pair_bias(z_trunk, relpos_table, w_pair_in, w_z_up, w_z_down, w_pair_bias)
    key_valid = jnp.arange(N_TOKENS) < N_VALID
    joined = layer_norm(jnp.concatenate([s_trunk, s_inputs], axis=-1)).astype(jnp.bfloat16)
    s_base = jnp.dot(joined, w_single, preferred_element_type=jnp.float32)
    x_state = sigmas[0] * x_noise
    for step_idx in range(STEPS):
        sigma_prev = sigmas[step_idx]
        t_hat = sigma_prev * (1.0 + GAMMA)
        x_noisy = x_state + NOISE_SCALE * jnp.sqrt(t_hat * t_hat - sigma_prev * sigma_prev) * step_noise[step_idx]
        single_ln = single_cond(s_base, t_hat, fourier_w, fourier_b, w_fourier, w_s_up, w_s_down)
        noise_var = t_hat * t_hat + SIGMA_DATA * SIGMA_DATA
        r_noisy = x_noisy / jnp.sqrt(noise_var)
        token_acts = jnp.sum(r_noisy[:, :, None] * w_in[None, :, :], axis=1) + jnp.dot(single_ln, w_s_tok, preferred_element_type=jnp.float32)
        for block_idx in range(BLOCKS):
            cond_proj = jnp.dot(single_ln, w_cond[block_idx], preferred_element_type=jnp.float32)
            normed = (jax.nn.sigmoid(cond_proj[:, :C_TOKEN]) * layer_norm(token_acts) + cond_proj[:, C_TOKEN:2 * C_TOKEN]).astype(jnp.bfloat16)
            qkvg_proj = jnp.dot(normed, w_qkvg[block_idx], preferred_element_type=jnp.float32)
            query_heads = qkvg_proj[:, :C_TOKEN].astype(jnp.bfloat16).reshape(N_TOKENS, HEADS, HEAD_DIM)
            key_heads = qkvg_proj[:, C_TOKEN:2 * C_TOKEN].astype(jnp.bfloat16).reshape(N_TOKENS, HEADS, HEAD_DIM)
            value_heads = qkvg_proj[:, 2 * C_TOKEN:3 * C_TOKEN].astype(jnp.bfloat16).reshape(N_TOKENS, HEADS, HEAD_DIM)
            scores = jnp.einsum("qhd,khd->hqk", query_heads.astype(jnp.float32), key_heads.astype(jnp.float32)) * HEAD_DIM ** -0.5 + bias_all[block_idx].astype(jnp.float32)
            scores = jnp.where(key_valid, scores, MASK_VALUE)
            attn_probs = jax.nn.softmax(scores, axis=-1).astype(jnp.bfloat16)
            attn_mix = jnp.einsum("hqk,khd->qhd", attn_probs.astype(jnp.float32), value_heads.astype(jnp.float32)).reshape(N_TOKENS, C_TOKEN)
            gated_mix = (jax.nn.sigmoid(qkvg_proj[:, 3 * C_TOKEN:]) * attn_mix).astype(jnp.bfloat16)
            attn_out = jnp.dot(gated_mix, w_attn_out[block_idx], preferred_element_type=jnp.float32)
            token_acts = token_acts + jax.nn.sigmoid(cond_proj[:, 2 * C_TOKEN:3 * C_TOKEN] + gate_bias[block_idx, 0]) * attn_out
            normed = (jax.nn.sigmoid(cond_proj[:, 3 * C_TOKEN:4 * C_TOKEN]) * layer_norm(token_acts) + cond_proj[:, 4 * C_TOKEN:5 * C_TOKEN]).astype(jnp.bfloat16)
            hidden = jnp.dot(normed, w_up[block_idx], preferred_element_type=jnp.float32)
            gated_act = (jax.nn.silu(hidden[:, :2 * C_TOKEN]) * hidden[:, 2 * C_TOKEN:]).astype(jnp.bfloat16)
            token_acts = token_acts + jax.nn.sigmoid(cond_proj[:, 5 * C_TOKEN:] + gate_bias[block_idx, 1]) * jnp.dot(gated_act, w_down[block_idx], preferred_element_type=jnp.float32)
        r_update = jnp.dot(layer_norm(token_acts).astype(jnp.bfloat16), w_out, preferred_element_type=jnp.float32)
        denoised = (SIGMA_DATA * SIGMA_DATA / noise_var) * x_noisy + (t_hat * SIGMA_DATA / jnp.sqrt(noise_var)) * r_update
        x_state = x_noisy + STEP_SCALE * (sigmas[step_idx + 1] - t_hat) * (x_noisy - denoised) / t_hat
    return x_state
```

```python
import math
import functools
import jax
import jax.numpy as jnp
from jax import lax
from jax.experimental import pallas as pl
from jax.experimental.pallas import tpu as pltpu
from jax.sharding import PartitionSpec as P

EPS = 1e-5
LOG2E = math.log2(math.e)


def spread(n, sub):
    rows = lax.broadcasted_iota(jnp.int32, (n * sub, n), 0)
    cols = lax.broadcasted_iota(jnp.int32, (n * sub, n), 1)
    return ((rows >= cols * sub) & (rows < (cols + 1) * sub)).astype(jnp.bfloat16)


def expand(weight, sub):
    n_out, n_in = weight.shape
    tall = jnp.dot(spread(n_out, sub), weight, preferred_element_type=jnp.float32).astype(jnp.bfloat16)
    full = lax.dot_general(tall, spread(n_in, sub), (((1,), (1,)), ((), ())), preferred_element_type=jnp.float32)
    rows = lax.broadcasted_iota(jnp.int32, full.shape, 0) & (sub - 1)
    cols = lax.broadcasted_iota(jnp.int32, full.shape, 1) & (sub - 1)
    return jnp.where(rows == cols, full, 0.0).astype(jnp.bfloat16)


def norm_major(values, sub):
    parts = values.reshape(values.shape[0] // sub, sub, values.shape[1])
    inv = 1.0 / parts.shape[0]
    centered = parts - jnp.sum(parts, axis=0, keepdims=True) * inv
    variance = jnp.sum(centered * centered, axis=0, keepdims=True) * inv
    return (centered * lax.rsqrt(variance + EPS)).reshape(values.shape)


def silu(h):
    half = 0.5 * h
    return half + half * jnp.tanh(half)


def bias_kernel(chunk, tok_name, z_ref, rel_ref, pin_ref, zup_ref, zdown_ref, pb_ref, out_ref, win_s, wup_s, wdown_s, wpb_s, perm_s, rel_s, relsum_s):
    sub = 8
    rows, c_pair, n_tok = z_ref.shape[0], z_ref.shape[1], z_ref.shape[2]
    n_layers = zup_ref.shape[0]
    n_bins = rel_ref.shape[1]
    clip = (n_bins - 1) // 2
    lanes = 128
    n_var = rel_s.shape[0]
    tile = c_pair * sub
    step = pl.program_id(0)

    @pl.when(step == 0)
    def _():
        pin = pin_ref[...]
        win_s[:, :tile] = expand(pin[:, :c_pair], sub)
        win_s[:, tile:] = expand(pin[:, c_pair:], sub)
        for layer in range(n_layers):
            wup_s[layer] = expand(zup_ref[layer], sub)
            wdown_s[layer] = expand(zdown_ref[layer], sub)
        wpb_s[...] = expand(pb_ref[...], sub)
        rows_i = lax.broadcasted_iota(jnp.int32, (tile, tile), 0)
        cols_i = lax.broadcasted_iota(jnp.int32, (tile, tile), 1)
        src = (rows_i & (sub - 1)) * c_pair + (rows_i >> 3)
        perm_s[...] = (src == cols_i).astype(jnp.bfloat16)
        tall = jnp.dot(spread(c_pair, sub), rel_ref[...], preferred_element_type=jnp.float32).astype(jnp.bfloat16)
        n_diag = 128
        tab = jnp.zeros((tile, n_diag), jnp.float32)
        bin_i = lax.broadcasted_iota(jnp.int32, (n_bins, n_diag), 0)
        diag_i = lax.broadcasted_iota(jnp.int32, (n_bins, n_diag), 1)
        row_s = lax.broadcasted_iota(jnp.int32, (tile, n_diag), 0) & (sub - 1)
        for s in range(sub):
            pick = (bin_i == jnp.clip(diag_i - (sub - 1) + s, 0, n_bins - 1)).astype(jnp.bfloat16)
            cand = jnp.dot(tall, pick, preferred_element_type=jnp.float32)
            tab = jnp.where(row_s == s, cand, tab)
        tab = tab.astype(jnp.bfloat16)

        def fill(v, carry):
            delta = sub * (v - 5)
            k = lax.broadcasted_iota(jnp.int32, (n_diag, lanes), 0)
            j = lax.broadcasted_iota(jnp.int32, (n_diag, lanes), 1)
            want = jnp.clip(delta - j + clip + sub - 1, 0, n_bins + sub - 2)
            plane = jnp.dot(tab, (k == want).astype(jnp.bfloat16), preferred_element_type=jnp.float32)
            rel_s[v] = plane
            relsum_s[v] = jnp.sum(plane.reshape(c_pair, sub, lanes), axis=0)
            return carry

        lax.fori_loop(0, n_var, fill, 0)

    row0 = lax.axis_index(tok_name) * (rows * pl.num_programs(0)) + step * rows

    def body(it, carry):
        n_chunks = n_tok // chunk
        group = it // n_chunks
        col0 = (it % n_chunks) * chunk
        r0 = group * sub
        zb = z_ref[pl.ds(r0, sub), :, pl.ds(pl.multiple_of(col0, chunk), chunk)].reshape(tile, chunk)
        z = jnp.dot(perm_s[...], zb, preferred_element_type=jnp.float32)
        rels, sums = [], []
        for part in range(chunk // lanes):
            delta = row0 + r0 - col0 - part * lanes
            v = jnp.clip(delta // sub + 5, 0, n_var - 1)
            rels.append(rel_s[v])
            sums.append(relsum_s[v])
        rel = jnp.concatenate(rels, axis=1).reshape(c_pair, sub, chunk)
        relsum = jnp.concatenate(sums, axis=1)
        z = z.reshape(c_pair, sub, chunk)
        inv = 1.0 / (2 * c_pair)
        mean = (jnp.sum(z, axis=0) + relsum) * inv
        zc = z - mean
        rc = rel - mean
        var = (jnp.sum(zc * zc, axis=0) + jnp.sum(rc * rc, axis=0)) * inv
        rs = lax.rsqrt(var + EPS)
        zn = (zc * rs).reshape(tile, chunk).astype(jnp.bfloat16)
        rn = (rc * rs).reshape(tile, chunk).astype(jnp.bfloat16)
        cond = jnp.dot(win_s[...], jnp.concatenate([zn, rn], axis=0), preferred_element_type=jnp.float32)
        for layer in range(n_layers):
            xn = norm_major(cond, sub).astype(jnp.bfloat16)
            h = jnp.dot(wup_s[layer], xn, preferred_element_type=jnp.float32)
            half = h.shape[0] // 2
            act = (silu(h[:half]) * h[half:]).astype(jnp.bfloat16)
            cond = cond + jnp.dot(wdown_s[layer], act, preferred_element_type=jnp.float32)
        xn = norm_major(cond, sub).astype(jnp.bfloat16)
        bias = jnp.dot(wpb_s[...], xn, preferred_element_type=jnp.float32)
        bias = bias.astype(jnp.bfloat16).astype(jnp.float32)
        out_ref[:, pl.ds(pl.multiple_of(r0, sub), sub), pl.ds(pl.multiple_of(col0, chunk), chunk)] = bias.reshape(-1, sub, chunk)
        return carry

    lax.fori_loop(0, (rows // sub) * (n_tok // chunk), body, 0)


def pair_bias(z_rows, relpos_table, w_pair_in, w_z_up, w_z_down, w_pair_bias, chunk=256, rows=16):
    tok_rows, n_tok, c_pair = z_rows.shape
    n_blocks, _, n_heads = w_pair_bias.shape
    n_layers = w_z_up.shape[0]
    width = w_z_up.shape[2]
    sub = 8
    n_var = 26
    zt = jnp.transpose(z_rows, (0, 2, 1))
    whole = lambda a: pl.BlockSpec(a.shape, lambda i, n=a.ndim: (0,) * n)
    ops = [relpos_table.T, w_pair_in.T, jnp.transpose(w_z_up, (0, 2, 1)), jnp.transpose(w_z_down, (0, 2, 1)), jnp.transpose(w_pair_bias, (0, 2, 1)).reshape(n_blocks * n_heads, c_pair)]
    out = pl.pallas_call(
        functools.partial(bias_kernel, chunk, "tok"),
        grid=(tok_rows // rows,),
        in_specs=[pl.BlockSpec((rows, c_pair, n_tok), lambda i: (i, 0, 0))] + [whole(a) for a in ops],
        out_specs=pl.BlockSpec((n_blocks * n_heads, rows, n_tok), lambda i: (0, i, 0)),
        out_shape=jax.ShapeDtypeStruct((n_blocks * n_heads, tok_rows, n_tok), jnp.float32),
        scratch_shapes=[
            pltpu.VMEM((c_pair * sub, 2 * c_pair * sub), jnp.bfloat16),
            pltpu.VMEM((n_layers, width * sub, c_pair * sub), jnp.bfloat16),
            pltpu.VMEM((n_layers, c_pair * sub, width // 2 * sub), jnp.bfloat16),
            pltpu.VMEM((n_blocks * n_heads * sub, c_pair * sub), jnp.bfloat16),
            pltpu.VMEM((c_pair * sub, c_pair * sub), jnp.bfloat16),
            pltpu.VMEM((n_var, c_pair * sub, 128), jnp.float32),
            pltpu.VMEM((n_var, sub, 128), jnp.float32),
        ],
        compiler_params=pltpu.CompilerParams(dimension_semantics=("arbitrary",), vmem_limit_bytes=48 * 1024 * 1024),
        cost_estimate=pl.CostEstimate(flops=10**10, bytes_accessed=10**7, transcendentals=10**7),
        name="pair_bias",
    )(zt, *ops)
    return out.reshape(n_blocks, n_heads, tok_rows, n_tok)


SIGMA_DATA = 16.0
GAMMA = 0.8
NOISE_SCALE = 1.003
STEP_SCALE = 1.5
MASK_VALUE = -1e9


def layer_norm(values):
    values = values.astype(jnp.float32)
    centered = values - jnp.mean(values, axis=-1, keepdims=True)
    variance = jnp.mean(centered * centered, axis=-1, keepdims=True)
    return centered * lax.rsqrt(variance + 1e-5)


def transition(values, w_up_one, w_down_one):
    hidden = jnp.dot(layer_norm(values).astype(jnp.bfloat16), w_up_one, preferred_element_type=jnp.float32)
    half_width = hidden.shape[-1] // 2
    gated_act = (jax.nn.silu(hidden[..., :half_width]) * hidden[..., half_width:]).astype(jnp.bfloat16)
    return values + jnp.dot(gated_act, w_down_one, preferred_element_type=jnp.float32)


def single_cond(s_base, t_hat, fourier_w, fourier_b, w_fourier, w_s_up, w_s_down):
    noise_level = 0.25 * jnp.log(t_hat / SIGMA_DATA)
    fourier_feat = jnp.cos(2.0 * math.pi * (noise_level * fourier_w + fourier_b))
    single = s_base + jnp.dot(layer_norm(fourier_feat[None, :]).astype(jnp.bfloat16), w_fourier, preferred_element_type=jnp.float32)
    for layer_idx in range(w_s_up.shape[0]):
        single = transition(single, w_s_up[layer_idx], w_s_down[layer_idx])
    return layer_norm(single).astype(jnp.bfloat16)


def solution(mesh):
    part_axes = ("sample", "tok")

    def local_run(s_trunk, s_inputs, z_trunk, x_noise, step_noise, sigmas, relpos_table, w_pair_in, w_z_up, w_z_down, w_pair_bias, w_single, fourier_w, fourier_b, w_fourier, w_s_up, w_s_down, w_in, w_s_tok, w_cond, gate_bias, w_qkvg, w_attn_out, w_up, w_down, w_out):
        tok_rows = z_trunk.shape[0]
        n_tok = z_trunk.shape[1]
        n_valid = n_tok - tok_rows // 4
        n_steps = step_noise.shape[0]
        n_blocks = w_qkvg.shape[0]
        c_token = w_qkvg.shape[1]
        n_heads = w_pair_bias.shape[2]
        head_dim = c_token // n_heads
        score_scale = head_dim ** -0.5
        bias_all = pair_bias(z_trunk, relpos_table, w_pair_in, w_z_up, w_z_down, w_pair_bias)
        key_valid = jnp.arange(n_tok) < n_valid
        joined = layer_norm(jnp.concatenate([s_trunk, s_inputs], axis=-1)).astype(jnp.bfloat16)
        s_base = jnp.dot(joined, w_single, preferred_element_type=jnp.float32)
        x_state = sigmas[0] * x_noise
        for step_idx in range(n_steps):
            sigma_prev = sigmas[step_idx]
            t_hat = sigma_prev * (1.0 + GAMMA)
            x_noisy = x_state + NOISE_SCALE * jnp.sqrt(t_hat * t_hat - sigma_prev * sigma_prev) * step_noise[step_idx]
            single_ln = single_cond(s_base, t_hat, fourier_w, fourier_b, w_fourier, w_s_up, w_s_down)
            noise_var = t_hat * t_hat + SIGMA_DATA * SIGMA_DATA
            r_noisy = x_noisy / jnp.sqrt(noise_var)
            token_acts = jnp.sum(r_noisy[:, :, None] * w_in[None, :, :], axis=1) + jnp.dot(single_ln, w_s_tok, preferred_element_type=jnp.float32)
            for block_idx in range(n_blocks):
                cond_proj = jnp.dot(single_ln, w_cond[block_idx], preferred_element_type=jnp.float32)
                normed = (jax.nn.sigmoid(cond_proj[:, :c_token]) * layer_norm(token_acts) + cond_proj[:, c_token:2 * c_token]).astype(jnp.bfloat16)
                qkvg_proj = jnp.dot(normed, w_qkvg[block_idx], preferred_element_type=jnp.float32)
                query_heads = qkvg_proj[:, :c_token].astype(jnp.bfloat16).reshape(tok_rows, n_heads, head_dim)
                kv_local = qkvg_proj[:, c_token:3 * c_token].astype(jnp.bfloat16)
                kv_all = lax.all_gather(kv_local, "tok", axis=0, tiled=True)
                key_heads = kv_all[:, :c_token].reshape(n_tok, n_heads, head_dim)
                value_heads = kv_all[:, c_token:].reshape(n_tok, n_heads, head_dim)
                scores = jnp.einsum("qhd,khd->hqk", query_heads, key_heads, preferred_element_type=jnp.float32) * score_scale + bias_all[block_idx]
                scores = jnp.where(key_valid, scores, MASK_VALUE)
                attn_probs = jax.nn.softmax(scores, axis=-1).astype(jnp.bfloat16)
                attn_mix = jnp.einsum("hqk,khd->qhd", attn_probs, value_heads, preferred_element_type=jnp.float32).reshape(tok_rows, c_token)
                gated_mix = (jax.nn.sigmoid(qkvg_proj[:, 3 * c_token:]) * attn_mix).astype(jnp.bfloat16)
                attn_out = jnp.dot(gated_mix, w_attn_out[block_idx], preferred_element_type=jnp.float32)
                token_acts = token_acts + jax.nn.sigmoid(cond_proj[:, 2 * c_token:3 * c_token] + gate_bias[block_idx, 0]) * attn_out
                normed = (jax.nn.sigmoid(cond_proj[:, 3 * c_token:4 * c_token]) * layer_norm(token_acts) + cond_proj[:, 4 * c_token:5 * c_token]).astype(jnp.bfloat16)
                hidden = jnp.dot(normed, w_up[block_idx], preferred_element_type=jnp.float32)
                gated_act = (jax.nn.silu(hidden[:, :2 * c_token]) * hidden[:, 2 * c_token:]).astype(jnp.bfloat16)
                token_acts = token_acts + jax.nn.sigmoid(cond_proj[:, 5 * c_token:] + gate_bias[block_idx, 1]) * jnp.dot(gated_act, w_down[block_idx], preferred_element_type=jnp.float32)
            r_update = jnp.dot(layer_norm(token_acts).astype(jnp.bfloat16), w_out, preferred_element_type=jnp.float32)
            denoised = (SIGMA_DATA * SIGMA_DATA / noise_var) * x_noisy + (t_hat * SIGMA_DATA / jnp.sqrt(noise_var)) * r_update
            x_state = x_noisy + STEP_SCALE * (sigmas[step_idx + 1] - t_hat) * (x_noisy - denoised) / t_hat
        return x_state

    in_specs = (P("tok", None), P("tok", None), P("tok", None, None), P(part_axes, None), P(None, part_axes, None)) + (P(),) * 21
    return jax.shard_map(local_run, mesh=mesh, in_specs=in_specs, out_specs=P(part_axes, None), check_vma=False)
```

```python
import functools
import math
import jax
import jax.numpy as jnp
from jax import lax
from jax.experimental import pallas as pl
from jax.experimental.pallas import tpu as pltpu
from jax.sharding import PartitionSpec as P

SIGMA_DATA = 16.0
GAMMA = 0.8
NOISE_SCALE = 1.003
STEP_SCALE = 1.5
MASK_VALUE = -1e9
EPS = 1e-5
LOG2E = math.log2(math.e)
LANES = 128
SUB = 8
CHUNK = 256
F32 = jnp.float32
BF16 = jnp.bfloat16


def dot(a, b):
    return jnp.dot(a, b, preferred_element_type=F32)


def dot_t(a, b):
    return lax.dot_general(a, b, (((1,), (1,)), ((), ())), preferred_element_type=F32)


def spread(n):
    rows = lax.broadcasted_iota(jnp.int32, (n * SUB, n), 0)
    cols = lax.broadcasted_iota(jnp.int32, (n * SUB, n), 1)
    return (rows // SUB == cols).astype(BF16)


def expand_tall(tall):
    full = dot_t(tall.astype(BF16), spread(tall.shape[1]))
    rows = lax.broadcasted_iota(jnp.int32, full.shape, 0) & (SUB - 1)
    cols = lax.broadcasted_iota(jnp.int32, full.shape, 1) & (SUB - 1)
    return jnp.where(rows == cols, full, 0.0)


def expand(weight):
    return expand_tall(dot(spread(weight.shape[0]), weight)).astype(BF16)


def norm_major(values):
    parts = values.reshape(values.shape[0] // SUB, SUB, values.shape[1])
    inv = 1.0 / parts.shape[0]
    centered = parts - jnp.sum(parts, axis=0, keepdims=True) * inv
    variance = jnp.sum(centered * centered, axis=0, keepdims=True) * inv
    return (centered * lax.rsqrt(variance + EPS)).reshape(values.shape).astype(BF16)


def norm_rows(values):
    inv = 1.0 / values.shape[-1]
    centered = values - jnp.sum(values, axis=-1, keepdims=True) * inv
    variance = jnp.sum(centered * centered, axis=-1, keepdims=True) * inv
    return centered * lax.rsqrt(variance + EPS)


def sigmoid(h):
    return 0.5 + 0.5 * jnp.tanh(0.5 * h)


def silu(h):
    half = 0.5 * h
    return half + half * jnp.tanh(half)


def kernel(
    axis, n_peers,
    sig_ref, z_hbm, rel_ref, pin_ref, zup_ref, zdown_ref, pb_ref,
    st_ref, si_ref, x_ref, noise_ref, wsingle_ref, fw_ref, fb_ref, wfour_ref, wsup_ref, wsdown_ref,
    win_ref, wstok_ref, wcond_ref, gbias_ref, wqkvg_ref, wao_ref, wup_ref, wdown_ref, wout_ref,
    out_ref,
    z_s, bias_s, pwin_s, pwup_s, pwdown_s, pwpb_s, perm_s, rel_s, relsum_s,
    zp_s, cond_ss, held_ss, act_ss,
    base_s, four_s, astok_s, gate_s, acts_s, xs_s, y_s,
    z_sem, send_sem, recv_sem,
):
    me = lax.axis_index(axis)
    tok_rows, c_pair, n_tok = z_hbm.shape
    n_layers = zup_ref.shape[0]
    n_bins = rel_ref.shape[1]
    clip = (n_bins - 1) // 2
    n_blocks, n_heads = pb_ref.shape[0], pb_ref.shape[1]
    c_token = st_ref.shape[1]
    head_dim = c_token // n_heads
    n_steps = noise_ref.shape[0]
    n_valid = n_tok - tok_rows // 4
    tile = c_pair * SUB
    n_var = rel_s.shape[0]
    low = (clip + SUB) // SUB

    z_copy = pltpu.make_async_copy(z_hbm, z_s, z_sem)
    z_copy.start()
    barrier = pltpu.get_barrier_semaphore()
    for off in range(1, n_peers):
        pl.semaphore_signal(barrier, inc=1, device_id={axis: lax.rem(me + off, n_peers)}, device_id_type=pl.DeviceIdType.MESH)

    row = lax.broadcasted_iota(jnp.int32, (SUB, 1), 0)
    t_col = jnp.full((SUB, 1), sig_ref[0] * (1.0 + GAMMA), F32)
    for k in range(1, n_steps):
        t_col = jnp.where(row == k, sig_ref[k] * (1.0 + GAMMA), t_col)
    level = 0.25 * jnp.log(t_col / SIGMA_DATA)
    feat = jnp.cos(2.0 * math.pi * (level * fw_ref[...] + fb_ref[...]))
    four_s[...] = dot(norm_rows(feat).astype(BF16), wfour_ref[...])
    joined = norm_rows(jnp.concatenate([st_ref[...].astype(F32), si_ref[...].astype(F32)], axis=-1)).astype(BF16)
    base_s[...] = dot(joined, wsingle_ref[...])

    def condition(k):
        single = base_s[...] + four_s[pl.ds(k, 1), :]
        for layer in range(wsup_ref.shape[0]):
            h = dot(norm_rows(single).astype(BF16), wsup_ref[layer])
            half = h.shape[1] // 2
            act = (silu(h[:, :half]) * h[:, half:]).astype(BF16)
            single = single + dot(act, wsdown_ref[layer])
        u = norm_rows(single).astype(BF16)
        astok_s[k] = dot(u, wstok_ref[...])
        for b in range(n_blocks):
            cond = dot(u, wcond_ref[b])
            part = lambda i: cond[:, i * c_token:(i + 1) * c_token]
            gate_s[k, b, 0] = sigmoid(part(0))
            gate_s[k, b, 1] = part(1)
            gate_s[k, b, 2] = sigmoid(part(2) + gbias_ref[b, 0:1, :])
            gate_s[k, b, 3] = sigmoid(part(3))
            gate_s[k, b, 4] = part(4)
            gate_s[k, b, 5] = sigmoid(part(5) + gbias_ref[b, 1:2, :])

    def copies(r):
        out = []
        for off in range(1, n_peers):
            peer = lax.rem(me + off, n_peers)
            out.append(pltpu.make_async_remote_copy(
                src_ref=y_s.at[r, me], dst_ref=y_s.at[r, me],
                send_sem=send_sem.at[r, off - 1], recv_sem=recv_sem.at[r, off - 1],
                device_id={axis: peer}, device_id_type=pl.DeviceIdType.MESH))
        return out

    def noisy(k):
        c = jnp.full((1, tok_rows), sig_ref[k], F32)
        t = c * (1.0 + GAMMA)
        xn = xs_s[...] + NOISE_SCALE * jnp.sqrt(t * t - c * c) * noise_ref[k]
        return xn, t, t * t + SIGMA_DATA * SIGMA_DATA

    def begin(k):
        xn, t, var = noisy(k)
        r = xn / jnp.sqrt(var)
        cols = jnp.transpose(jnp.concatenate([r, jnp.zeros((SUB - r.shape[0], r.shape[1]), F32)], axis=0))
        acts = astok_s[k]
        lin = cols[:, 0:1] * win_ref[0:1, :]
        for d in range(1, r.shape[0]):
            lin = lin + cols[:, d:d + 1] * win_ref[d:d + 1, :]
        acts_s[...] = lin + acts

    def send(k, b, r):
        y = (gate_s[k, b, 0] * norm_rows(acts_s[...]) + gate_s[k, b, 1]).astype(BF16)
        y_s[r, me] = y
        for copy in copies(r):
            copy.start()

    condition(0)
    xs_s[...] = sig_ref[0] * x_ref[...]
    begin(0)
    pl.semaphore_wait(barrier, n_peers - 1)
    send(0, 0, 0)

    pin = pin_ref[...]
    pwin_s[:, :tile] = expand(pin[:, :c_pair])
    pwin_s[:, tile:] = expand(pin[:, c_pair:])
    for layer in range(n_layers):
        up = zup_ref[layer]
        width = up.shape[1]
        full = expand_tall(dot_t(spread(width), up))
        gate_rows = lax.broadcasted_iota(jnp.int32, full.shape, 0) < (width // 2) * SUB
        pwup_s[layer] = jnp.where(gate_rows, 0.5 * full, full).astype(BF16)
        pwdown_s[layer] = expand(zdown_ref[layer])
    for b in range(n_blocks):
        pwpb_s[b * n_heads * SUB:(b + 1) * n_heads * SUB, :] = expand(pb_ref[b])
    rows_i = lax.broadcasted_iota(jnp.int32, (tile, tile), 0)
    cols_i = lax.broadcasted_iota(jnp.int32, (tile, tile), 1)
    perm_s[...] = ((rows_i & (SUB - 1)) * c_pair + rows_i // SUB == cols_i).astype(BF16)
    tall = dot(spread(c_pair), rel_ref[...]).astype(BF16)
    bin_i = lax.broadcasted_iota(jnp.int32, (n_bins, LANES), 0)
    diag_i = lax.broadcasted_iota(jnp.int32, (n_bins, LANES), 1)
    row_s = lax.broadcasted_iota(jnp.int32, (tile, LANES), 0) & (SUB - 1)
    tab = jnp.zeros((tile, LANES), F32)
    for s in range(SUB):
        pick = (bin_i == jnp.clip(diag_i - (SUB - 1) + s, 0, n_bins - 1)).astype(BF16)
        tab = jnp.where(row_s == s, dot(tall, pick), tab)
    tab = tab.astype(BF16)

    per = 2
    k_i = lax.broadcasted_iota(jnp.int32, (LANES, LANES), 0)
    j_i = lax.broadcasted_iota(jnp.int32, (LANES, LANES), 1)

    def fill(i, carry):
        picks = []
        for p in range(per):
            delta = SUB * (i * per + p - low)
            want = jnp.clip(delta - j_i + clip + SUB - 1, 0, n_bins + SUB - 2)
            picks.append((k_i == want).astype(BF16))
        planes = dot(tab, jnp.concatenate(picks, axis=1))
        for p in range(per):
            plane = planes[:, p * LANES:(p + 1) * LANES]
            rel_s[i * per + p] = plane
            relsum_s[i * per + p] = jnp.sum(plane.reshape(c_pair, SUB, LANES), axis=0)
        return carry

    lax.fori_loop(0, n_var // per, fill, 0)
    z_copy.wait()

    n_chunks = n_tok // CHUNK
    total = (tok_rows // SUB) * n_chunks
    depth = 2 + 2 * n_layers

    def place(it, lag):
        idx = jnp.clip(it - lag, 0, total - 1)
        return (idx // n_chunks) * SUB, (idx % n_chunks) * CHUNK

    def trip(it, carry):
        r0, c0 = place(it, depth)
        bias = dot(pwpb_s[...], norm_major(cond_ss[n_layers]))
        bias = bias.astype(BF16).astype(F32) * LOG2E
        bias_s[:, pl.ds(pl.multiple_of(r0, SUB), SUB), pl.ds(pl.multiple_of(c0, CHUNK), CHUNK)] = bias.reshape(n_blocks * n_heads, SUB, CHUNK)
        for layer in reversed(range(n_layers)):
            cond_ss[layer + 1] = held_ss[layer] + dot(pwdown_s[layer], act_ss[layer])
            cond = cond_ss[layer]
            h = dot(pwup_s[layer], norm_major(cond))
            half = h.shape[0] // 2
            gate = h[:half]
            act_ss[layer] = ((gate + gate * jnp.tanh(gate)) * h[half:]).astype(BF16)
            held_ss[layer] = cond
        r0, c0 = place(it, 1)
        z = zp_s[...].reshape(c_pair, SUB, CHUNK)
        rels, sums = [], []
        for part in range(CHUNK // LANES):
            delta = me * tok_rows + r0 - c0 - part * LANES
            v = jnp.clip(delta // SUB + low, 0, n_var - 1)
            rels.append(rel_s[v])
            sums.append(relsum_s[v])
        rel = jnp.concatenate(rels, axis=1).reshape(c_pair, SUB, CHUNK)
        inv = 1.0 / (2 * c_pair)
        mean = (jnp.sum(z, axis=0) + jnp.concatenate(sums, axis=1)) * inv
        zc = z - mean
        rc = rel - mean
        var = (jnp.sum(zc * zc, axis=0) + jnp.sum(rc * rc, axis=0)) * inv
        rs = lax.rsqrt(var + EPS)
        zn = (zc * rs).reshape(tile, CHUNK).astype(BF16)
        rn = (rc * rs).reshape(tile, CHUNK).astype(BF16)
        cond_ss[0] = dot(pwin_s[...], jnp.concatenate([zn, rn], axis=0))
        r0, c0 = place(it, 0)
        zb = z_s[pl.ds(r0, SUB), :, pl.ds(pl.multiple_of(c0, CHUNK), CHUNK)].reshape(tile, CHUNK)
        zp_s[...] = dot(perm_s[...], zb)
        return carry

    zp_s[...] = jnp.zeros(zp_s.shape, F32)
    cond_ss[...] = jnp.zeros(cond_ss.shape, F32)
    held_ss[...] = jnp.zeros(held_ss.shape, F32)
    act_ss[...] = jnp.zeros(act_ss.shape, BF16)
    lax.fori_loop(0, total + depth, trip, 0)

    lane = lax.broadcasted_iota(jnp.int32, (1, c_token), 1) // head_dim
    key_ok = lax.broadcasted_iota(jnp.int32, (1, LANES), 1) + (n_tok - LANES) < n_valid
    scale = head_dim ** -0.5 * LOG2E

    def block(k, b):
        r = k * n_blocks + b
        wq = lambda i: wqkvg_ref[b, :, i * c_token:(i + 1) * c_token]
        y = y_s[r, me]
        q = dot(y, wq(0)).astype(BF16)
        g = sigmoid(dot(y, wq(3)))
        q_heads = jnp.concatenate([jnp.where(lane == h, q, jnp.zeros_like(q)) for h in range(n_heads)], axis=0)
        for copy in copies(r):
            copy.wait_recv()
        y_all = y_s[r].reshape(n_tok, c_token)
        keys = dot(y_all, wq(1)).astype(BF16)
        values = dot(y_all, wq(2)).astype(BF16)
        scores = dot_t(q_heads, keys)
        probs = []
        for h in range(n_heads):
            sc = scores[h * tok_rows:(h + 1) * tok_rows] * scale + bias_s[b * n_heads + h]
            sc = jnp.concatenate([sc[:, :n_tok - LANES], jnp.where(key_ok, sc[:, n_tok - LANES:], MASK_VALUE * LOG2E)], axis=1)
            e = jnp.exp2(sc - jnp.max(sc, axis=1, keepdims=True))
            probs.append((e * (1.0 / jnp.sum(e, axis=1, keepdims=True))).astype(BF16))
        mixed = dot(jnp.concatenate(probs, axis=0), values)
        mix = mixed[:tok_rows]
        for h in range(1, n_heads):
            mix = jnp.where(lane == h, mixed[h * tok_rows:(h + 1) * tok_rows], mix)
        attn = dot((g * mix).astype(BF16), wao_ref[b])
        acts = acts_s[...] + gate_s[k, b, 2] * attn
        normed = (gate_s[k, b, 3] * norm_rows(acts) + gate_s[k, b, 4]).astype(BF16)
        h = dot(normed, wup_ref[b])
        half = h.shape[1] // 2
        act = (silu(h[:, :half]) * h[:, half:]).astype(BF16)
        acts_s[...] = acts + gate_s[k, b, 5] * dot(act, wdown_ref[b])
        for copy in copies(r):
            copy.wait_send()

    def step(k, carry):
        @pl.when(k > 0)
        def _():
            begin(k)
            send(k, 0, k * n_blocks)

        block(k, 0)
        for b in range(1, n_blocks):
            send(k, b, k * n_blocks + b)

            if b == 1:
                @pl.when(k == 0)
                def _():
                    for later in range(1, n_steps):
                        condition(later)

            block(k, b)
        xn, t, var = noisy(k)
        update = dot_t(wout_ref[...], norm_rows(acts_s[...]).astype(BF16))
        denoised = (SIGMA_DATA * SIGMA_DATA / var) * xn + (t * SIGMA_DATA / jnp.sqrt(var)) * update
        xs_s[...] = xn + STEP_SCALE * (sig_ref[k + 1] - t) * (xn - denoised) / t
        return carry

    lax.fori_loop(0, n_steps, step, 0)
    out_ref[...] = xs_s[...]


def solution(mesh):
    part_axes = ("sample", "tok")
    n_peers = mesh.shape["tok"]

    def local_run(s_trunk, s_inputs, z_trunk, x_noise, step_noise, sigmas, relpos_table, w_pair_in, w_z_up, w_z_down, w_pair_bias, w_single, fourier_w, fourier_b, w_fourier, w_s_up, w_s_down, w_in, w_s_tok, w_cond, gate_bias, w_qkvg, w_attn_out, w_up, w_down, w_out):
        tok_rows, n_tok, c_pair = z_trunk.shape
        n_steps, _, n_dim = step_noise.shape
        n_blocks, _, n_heads = w_pair_bias.shape
        n_layers, _, width = w_z_up.shape
        c_token = w_qkvg.shape[1]
        clip = (relpos_table.shape[0] - 1) // 2
        tile = c_pair * SUB
        n_var = 2 * clip // SUB + LANES // SUB + 2
        n_rounds = n_steps * n_blocks
        swap = lambda a: jnp.swapaxes(a, -1, -2)
        ops = [
            sigmas, swap(z_trunk), swap(relpos_table), swap(w_pair_in), w_z_up, swap(w_z_down), swap(w_pair_bias),
            s_trunk, s_inputs, swap(x_noise), swap(step_noise), w_single, fourier_w[None, :], fourier_b[None, :], w_fourier, w_s_up, w_s_down,
            w_in, w_s_tok, w_cond, gate_bias, w_qkvg, w_attn_out, w_up, w_down, swap(w_out),
        ]
        specs = [pl.BlockSpec(memory_space=pltpu.SMEM), pl.BlockSpec(memory_space=pl.ANY)] + [pl.BlockSpec(memory_space=pltpu.VMEM)] * (len(ops) - 2)
        out = pl.pallas_call(
            functools.partial(kernel, "tok", n_peers),
            in_specs=specs,
            out_specs=pl.BlockSpec(memory_space=pltpu.VMEM),
            out_shape=jax.ShapeDtypeStruct((n_dim, tok_rows), F32),
            scratch_shapes=[
                pltpu.VMEM((tok_rows, c_pair, n_tok), BF16),
                pltpu.VMEM((n_blocks * n_heads, tok_rows, n_tok), F32),
                pltpu.VMEM((tile, 2 * tile), BF16),
                pltpu.VMEM((n_layers, width * SUB, tile), BF16),
                pltpu.VMEM((n_layers, tile, width // 2 * SUB), BF16),
                pltpu.VMEM((n_blocks * n_heads * SUB, tile), BF16),
                pltpu.VMEM((tile, tile), BF16),
                pltpu.VMEM((n_var, tile, LANES), F32),
                pltpu.VMEM((n_var, SUB, LANES), F32),
                pltpu.VMEM((tile, CHUNK), F32),
                pltpu.VMEM((n_layers + 1, tile, CHUNK), F32),
                pltpu.VMEM((n_layers, tile, CHUNK), F32),
                pltpu.VMEM((n_layers, width // 2 * SUB, CHUNK), BF16),
                pltpu.VMEM((tok_rows, c_token), F32),
                pltpu.VMEM((SUB, c_token), F32),
                pltpu.VMEM((n_steps, tok_rows, c_token), F32),
                pltpu.VMEM((n_steps, n_blocks, 6, tok_rows, c_token), F32),
                pltpu.VMEM((tok_rows, c_token), F32),
                pltpu.VMEM((n_dim, tok_rows), F32),
                pltpu.VMEM((n_rounds, n_peers, tok_rows, c_token), BF16),
                pltpu.SemaphoreType.DMA,
                pltpu.SemaphoreType.DMA((n_rounds, n_peers - 1)),
                pltpu.SemaphoreType.DMA((n_rounds, n_peers - 1)),
            ],
            compiler_params=pltpu.CompilerParams(collective_id=0, has_side_effects=True, vmem_limit_bytes=60 * 1024 * 1024),
            name="sampler",
        )(*ops)
        return swap(out)

    in_specs = (P("tok", None), P("tok", None), P("tok", None, None), P(part_axes, None), P(None, part_axes, None)) + (P(),) * 21
    return jax.shard_map(local_run, mesh=mesh, in_specs=in_specs, out_specs=P(part_axes, None), check_vma=False)
```

```python
import functools
import math
import jax
import jax.numpy as jnp
from jax import lax
from jax.experimental import pallas as pl
from jax.experimental.pallas import tpu as pltpu
from jax.sharding import PartitionSpec as P

SIGMA_DATA = 16.0
GAMMA = 0.8
NOISE_SCALE = 1.003
STEP_SCALE = 1.5
MASK_VALUE = -1e9
EPS = 1e-5
LOG2E = math.log2(math.e)
LANES = 128
SUB = 8
CHUNK = 256
UNROLL = 7
F32 = jnp.float32
BF16 = jnp.bfloat16


def dot(a, b):
    return jnp.dot(a, b, preferred_element_type=F32)


def dot_t(a, b):
    return lax.dot_general(a, b, (((1,), (1,)), ((), ())), preferred_element_type=F32)


def spread(n):
    rows = lax.broadcasted_iota(jnp.int32, (n * SUB, n), 0)
    cols = lax.broadcasted_iota(jnp.int32, (n * SUB, n), 1)
    return (rows // SUB == cols).astype(BF16)


def expand_tall(tall):
    full = dot_t(tall.astype(BF16), spread(tall.shape[1]))
    rows = lax.broadcasted_iota(jnp.int32, full.shape, 0) & (SUB - 1)
    cols = lax.broadcasted_iota(jnp.int32, full.shape, 1) & (SUB - 1)
    return jnp.where(rows == cols, full, 0.0)


def expand(weight):
    return expand_tall(dot(spread(weight.shape[0]), weight)).astype(BF16)


def norm_major(values):
    parts = values.reshape(values.shape[0] // SUB, SUB, values.shape[1])
    inv = 1.0 / parts.shape[0]
    centered = parts - jnp.sum(parts, axis=0, keepdims=True) * inv
    variance = jnp.sum(centered * centered, axis=0, keepdims=True) * inv
    return (centered * lax.rsqrt(variance + EPS)).reshape(values.shape).astype(BF16)


def norm_rows(values):
    inv = 1.0 / values.shape[-1]
    centered = values - jnp.sum(values, axis=-1, keepdims=True) * inv
    variance = jnp.sum(centered * centered, axis=-1, keepdims=True) * inv
    return centered * lax.rsqrt(variance + EPS)


def sigmoid(h):
    return 0.5 + 0.5 * jnp.tanh(0.5 * h)


def silu(h):
    half = 0.5 * h
    return half + half * jnp.tanh(half)


def kernel(
    axis, n_peers,
    sig_ref, z_hbm, rel_ref, pin_ref, zup_ref, zdown_ref, pb_ref,
    st_ref, si_ref, x_ref, noise_ref, wsingle_ref, fw_ref, fb_ref, wfour_ref, wsup_ref, wsdown_ref,
    win_ref, wstok_ref, wcond_ref, gbias_ref, wqkvg_ref, wao_ref, wup_ref, wdown_ref, wout_ref,
    out_ref,
    z_s, bias_s, pwin_s, pwup_s, pwdown_s, pwpb_s, perm_s, rel_s, relsum_s,
    zn_s, xn_ss, cond_ss, held_ss, act_ss,
    base_s, four_s, astok_s, gate_s, acts_s, xs_s, y_s,
    z_sem, send_sem, recv_sem,
):
    me = lax.axis_index(axis)
    tok_rows, c_pair, n_tok = z_hbm.shape
    n_layers = zup_ref.shape[0]
    n_bins = rel_ref.shape[1]
    clip = (n_bins - 1) // 2
    n_blocks, n_heads = pb_ref.shape[0], pb_ref.shape[1]
    c_token = st_ref.shape[1]
    head_dim = c_token // n_heads
    n_steps = noise_ref.shape[0]
    n_valid = n_tok - tok_rows // 4
    tile = c_pair * SUB
    n_var = rel_s.shape[0]
    low = (clip + SUB) // SUB

    z_copy = pltpu.make_async_copy(z_hbm, z_s, z_sem)
    z_copy.start()
    barrier = pltpu.get_barrier_semaphore()
    for off in range(1, n_peers):
        pl.semaphore_signal(barrier, inc=1, device_id={axis: lax.rem(me + off, n_peers)}, device_id_type=pl.DeviceIdType.MESH)

    row = lax.broadcasted_iota(jnp.int32, (SUB, 1), 0)
    t_col = jnp.full((SUB, 1), sig_ref[0] * (1.0 + GAMMA), F32)
    for k in range(1, n_steps):
        t_col = jnp.where(row == k, sig_ref[k] * (1.0 + GAMMA), t_col)
    level = 0.25 * jnp.log(t_col / SIGMA_DATA)
    feat = jnp.cos(2.0 * math.pi * (level * fw_ref[...] + fb_ref[...]))
    four_s[...] = dot(norm_rows(feat).astype(BF16), wfour_ref[...])
    joined = norm_rows(jnp.concatenate([st_ref[...].astype(F32), si_ref[...].astype(F32)], axis=-1)).astype(BF16)
    base_s[...] = dot(joined, wsingle_ref[...])

    def condition(k):
        single = base_s[...] + four_s[pl.ds(k, 1), :]
        for layer in range(wsup_ref.shape[0]):
            h = dot(norm_rows(single).astype(BF16), wsup_ref[layer])
            half = h.shape[1] // 2
            act = (silu(h[:, :half]) * h[:, half:]).astype(BF16)
            single = single + dot(act, wsdown_ref[layer])
        u = norm_rows(single).astype(BF16)
        astok_s[k] = dot(u, wstok_ref[...])
        for b in range(n_blocks):
            cond = dot(u, wcond_ref[b])
            part = lambda i: cond[:, i * c_token:(i + 1) * c_token]
            gate_s[k, b, 0] = sigmoid(part(0))
            gate_s[k, b, 1] = part(1)
            gate_s[k, b, 2] = sigmoid(part(2) + gbias_ref[b, 0:1, :])
            gate_s[k, b, 3] = sigmoid(part(3))
            gate_s[k, b, 4] = part(4)
            gate_s[k, b, 5] = sigmoid(part(5) + gbias_ref[b, 1:2, :])

    def copies(r):
        out = []
        for off in sorted(range(1, n_peers), key=lambda o: -min(o, n_peers - o)):
            peer = lax.rem(me + off, n_peers)
            out.append(pltpu.make_async_remote_copy(
                src_ref=y_s.at[r, me], dst_ref=y_s.at[r, me],
                send_sem=send_sem.at[r, off - 1], recv_sem=recv_sem.at[r, off - 1],
                device_id={axis: peer}, device_id_type=pl.DeviceIdType.MESH))
        return out

    def noisy(k):
        c = jnp.full((1, tok_rows), sig_ref[k], F32)
        t = c * (1.0 + GAMMA)
        xn = xs_s[...] + NOISE_SCALE * jnp.sqrt(t * t - c * c) * noise_ref[k]
        return xn, t, t * t + SIGMA_DATA * SIGMA_DATA

    def begin(k):
        xn, t, var = noisy(k)
        r = xn / jnp.sqrt(var)
        cols = jnp.transpose(jnp.concatenate([r, jnp.zeros((SUB - r.shape[0], r.shape[1]), F32)], axis=0))
        acts = astok_s[k]
        lin = cols[:, 0:1] * win_ref[0:1, :]
        for d in range(1, r.shape[0]):
            lin = lin + cols[:, d:d + 1] * win_ref[d:d + 1, :]
        acts_s[...] = lin + acts

    def send(k, b, r):
        y = (gate_s[k, b, 0] * norm_rows(acts_s[...]) + gate_s[k, b, 1]).astype(BF16)
        y_s[r, me] = y
        for copy in copies(r):
            copy.start()

    condition(0)
    xs_s[...] = sig_ref[0] * x_ref[...]
    begin(0)
    pl.semaphore_wait(barrier, n_peers - 1)
    send(0, 0, 0)

    pin = pin_ref[...]
    pwin_s[:, :tile] = expand(pin[:, :c_pair])
    pwin_s[:, tile:] = expand(pin[:, c_pair:])
    for layer in range(n_layers):
        up = zup_ref[layer]
        width = up.shape[1]
        full = expand_tall(dot_t(spread(width), up))
        gate_rows = lax.broadcasted_iota(jnp.int32, full.shape, 0) < (width // 2) * SUB
        pwup_s[layer] = jnp.where(gate_rows, 0.5 * full, full).astype(BF16)
        pwdown_s[layer] = expand(zdown_ref[layer])
    for b in range(n_blocks):
        pwpb_s[b * n_heads * SUB:(b + 1) * n_heads * SUB, :] = expand(pb_ref[b])
    rows_i = lax.broadcasted_iota(jnp.int32, (tile, tile), 0)
    cols_i = lax.broadcasted_iota(jnp.int32, (tile, tile), 1)
    perm_s[...] = ((rows_i & (SUB - 1)) * c_pair + rows_i // SUB == cols_i).astype(BF16)
    tall = dot(spread(c_pair), rel_ref[...]).astype(BF16)
    bin_i = lax.broadcasted_iota(jnp.int32, (n_bins, LANES), 0)
    diag_i = lax.broadcasted_iota(jnp.int32, (n_bins, LANES), 1)
    row_s = lax.broadcasted_iota(jnp.int32, (tile, LANES), 0) & (SUB - 1)
    tab = jnp.zeros((tile, LANES), F32)
    for s in range(SUB):
        pick = (bin_i == jnp.clip(diag_i - (SUB - 1) + s, 0, n_bins - 1)).astype(BF16)
        tab = jnp.where(row_s == s, dot(tall, pick), tab)
    tab = tab.astype(BF16)

    per = 2
    k_i = lax.broadcasted_iota(jnp.int32, (LANES, LANES), 0)
    j_i = lax.broadcasted_iota(jnp.int32, (LANES, LANES), 1)

    def fill(i, carry):
        picks = []
        for p in range(per):
            delta = SUB * (i * per + p - low)
            want = jnp.clip(delta - j_i + clip + SUB - 1, 0, n_bins + SUB - 2)
            picks.append((k_i == want).astype(BF16))
        planes = dot(tab, jnp.concatenate(picks, axis=1))
        for p in range(per):
            plane = planes[:, p * LANES:(p + 1) * LANES]
            rel_s[i * per + p] = plane
            relsum_s[i * per + p] = jnp.sum(plane.reshape(c_pair, SUB, LANES), axis=0)
        return carry

    lax.fori_loop(0, n_var // per, fill, 0)
    z_copy.wait()

    n_chunks = n_tok // CHUNK
    total = (tok_rows // SUB) * n_chunks
    depth = 2 + 2 * n_layers

    def trip(it):
        known = isinstance(it, int)

        def active(lag):
            return not known or 0 <= it - lag < total

        def place(lag):
            idx = it - lag
            r0, c0 = (idx // n_chunks) * SUB, (idx % n_chunks) * CHUNK
            return (r0, c0) if known else (pl.multiple_of(r0, SUB), pl.multiple_of(c0, CHUNK))

        if active(depth):
            r0, c0 = place(depth)
            bias = dot(pwpb_s[...], xn_ss[n_layers])
            bias = bias.astype(BF16).astype(F32) * LOG2E
            bias_s[:, pl.ds(r0, SUB), pl.ds(c0, CHUNK)] = bias.reshape(n_blocks * n_heads, SUB, CHUNK)
        for layer in reversed(range(n_layers)):
            if active(3 + 2 * layer):
                cond = held_ss[layer] + dot(pwdown_s[layer], act_ss[layer])
                xn_ss[layer + 1] = norm_major(cond)
            if active(2 + 2 * layer):
                h = dot(pwup_s[layer], xn_ss[layer])
                half = h.shape[0] // 2
                gate = h[:half]
                act_ss[layer] = ((gate + gate * jnp.tanh(gate)) * h[half:]).astype(BF16)
                held_ss[layer] = cond_ss[layer]
            if active(3 + 2 * layer) and layer + 1 < n_layers:
                cond_ss[layer + 1] = cond
        if active(1):
            cond = dot(pwin_s[...], zn_s[...])
            cond_ss[0] = cond
            xn_ss[0] = norm_major(cond)
        if active(0):
            r0, c0 = place(0)
            zb = z_s[pl.ds(r0, SUB), :, pl.ds(c0, CHUNK)].reshape(tile, CHUNK)
            z = dot(perm_s[...], zb).reshape(c_pair, SUB, CHUNK)
            rels, sums = [], []
            for part in range(CHUNK // LANES):
                delta = me * tok_rows + r0 - c0 - part * LANES
                v = jnp.clip(delta // SUB + low, 0, n_var - 1)
                rels.append(rel_s[v])
                sums.append(relsum_s[v])
            rel = jnp.concatenate(rels, axis=1).reshape(c_pair, SUB, CHUNK)
            inv = 1.0 / (2 * c_pair)
            mean = (jnp.sum(z, axis=0) + jnp.concatenate(sums, axis=1)) * inv
            zc = z - mean
            rc = rel - mean
            var = (jnp.sum(zc * zc, axis=0) + jnp.sum(rc * rc, axis=0)) * inv
            rs = lax.rsqrt(var + EPS)
            zn_s[:tile] = (zc * rs).reshape(tile, CHUNK).astype(BF16)
            zn_s[tile:] = (rc * rs).reshape(tile, CHUNK).astype(BF16)

    loops = (total - depth) // UNROLL

    def trips(i, carry):
        for j in range(UNROLL):
            trip(depth + i * UNROLL + j)
        return carry

    for it in range(depth):
        trip(it)
    lax.fori_loop(0, loops, trips, 0)
    for it in range(depth + loops * UNROLL, total + depth):
        trip(it)

    lane = lax.broadcasted_iota(jnp.int32, (1, c_token), 1) // head_dim
    key_ok = lax.broadcasted_iota(jnp.int32, (1, LANES), 1) + (n_tok - LANES) < n_valid
    scale = head_dim ** -0.5 * LOG2E

    def block(k, b):
        r = k * n_blocks + b
        wq = lambda i: wqkvg_ref[b, :, i * c_token:(i + 1) * c_token]
        y = y_s[r, me]
        q = dot(y, wq(0)).astype(BF16)
        g = sigmoid(dot(y, wq(3)))
        q_heads = jnp.concatenate([jnp.where(lane == h, q, jnp.zeros_like(q)) for h in range(n_heads)], axis=0)
        for copy in copies(r):
            copy.wait_recv()
        y_all = y_s[r].reshape(n_tok, c_token)
        keys = dot(y_all, wq(1)).astype(BF16)
        values = dot(y_all, wq(2)).astype(BF16)
        scores = dot_t(q_heads, keys)
        probs = []
        for h in range(n_heads):
            sc = scores[h * tok_rows:(h + 1) * tok_rows] * scale + bias_s[b * n_heads + h]
            sc = jnp.concatenate([sc[:, :n_tok - LANES], jnp.where(key_ok, sc[:, n_tok - LANES:], MASK_VALUE * LOG2E)], axis=1)
            e = jnp.exp2(sc - jnp.max(sc, axis=1, keepdims=True))
            probs.append((e * (1.0 / jnp.sum(e, axis=1, keepdims=True))).astype(BF16))
        mixed = dot(jnp.concatenate(probs, axis=0), values)
        mix = mixed[:tok_rows]
        for h in range(1, n_heads):
            mix = jnp.where(lane == h, mixed[h * tok_rows:(h + 1) * tok_rows], mix)
        attn = dot((g * mix).astype(BF16), wao_ref[b])
        acts = acts_s[...] + gate_s[k, b, 2] * attn
        normed = (gate_s[k, b, 3] * norm_rows(acts) + gate_s[k, b, 4]).astype(BF16)
        h = dot(normed, wup_ref[b])
        half = h.shape[1] // 2
        act = (silu(h[:, :half]) * h[:, half:]).astype(BF16)
        acts_s[...] = acts + gate_s[k, b, 5] * dot(act, wdown_ref[b])
        for copy in copies(r):
            copy.wait_send()

    def step(k, carry):
        @pl.when(k > 0)
        def _():
            begin(k)
            send(k, 0, k * n_blocks)

        block(k, 0)
        for b in range(1, n_blocks):
            send(k, b, k * n_blocks + b)

            if b == 1:
                @pl.when(k == 0)
                def _():
                    for later in range(1, n_steps):
                        condition(later)

            block(k, b)
        xn, t, var = noisy(k)
        update = dot_t(wout_ref[...], norm_rows(acts_s[...]).astype(BF16))
        denoised = (SIGMA_DATA * SIGMA_DATA / var) * xn + (t * SIGMA_DATA / jnp.sqrt(var)) * update
        xs_s[...] = xn + STEP_SCALE * (sig_ref[k + 1] - t) * (xn - denoised) / t
        return carry

    lax.fori_loop(0, n_steps, step, 0)
    out_ref[...] = xs_s[...]


def solution(mesh):
    part_axes = ("sample", "tok")
    n_peers = mesh.shape["tok"]

    def local_run(s_trunk, s_inputs, z_trunk, x_noise, step_noise, sigmas, relpos_table, w_pair_in, w_z_up, w_z_down, w_pair_bias, w_single, fourier_w, fourier_b, w_fourier, w_s_up, w_s_down, w_in, w_s_tok, w_cond, gate_bias, w_qkvg, w_attn_out, w_up, w_down, w_out):
        tok_rows, n_tok, c_pair = z_trunk.shape
        n_steps, _, n_dim = step_noise.shape
        n_blocks, _, n_heads = w_pair_bias.shape
        n_layers, _, width = w_z_up.shape
        c_token = w_qkvg.shape[1]
        clip = (relpos_table.shape[0] - 1) // 2
        tile = c_pair * SUB
        n_var = 2 * clip // SUB + LANES // SUB + 2
        n_rounds = n_steps * n_blocks
        swap = lambda a: jnp.swapaxes(a, -1, -2)
        ops = [
            sigmas, swap(z_trunk), swap(relpos_table), swap(w_pair_in), w_z_up, swap(w_z_down), swap(w_pair_bias),
            s_trunk, s_inputs, swap(x_noise), swap(step_noise), w_single, fourier_w[None, :], fourier_b[None, :], w_fourier, w_s_up, w_s_down,
            w_in, w_s_tok, w_cond, gate_bias, w_qkvg, w_attn_out, w_up, w_down, swap(w_out),
        ]
        specs = [pl.BlockSpec(memory_space=pltpu.SMEM), pl.BlockSpec(memory_space=pl.ANY)] + [pl.BlockSpec(memory_space=pltpu.VMEM)] * (len(ops) - 2)
        out = pl.pallas_call(
            functools.partial(kernel, "tok", n_peers),
            in_specs=specs,
            out_specs=pl.BlockSpec(memory_space=pltpu.VMEM),
            out_shape=jax.ShapeDtypeStruct((n_dim, tok_rows), F32),
            scratch_shapes=[
                pltpu.VMEM((tok_rows, c_pair, n_tok), BF16),
                pltpu.VMEM((n_blocks * n_heads, tok_rows, n_tok), F32),
                pltpu.VMEM((tile, 2 * tile), BF16),
                pltpu.VMEM((n_layers, width * SUB, tile), BF16),
                pltpu.VMEM((n_layers, tile, width // 2 * SUB), BF16),
                pltpu.VMEM((n_blocks * n_heads * SUB, tile), BF16),
                pltpu.VMEM((tile, tile), BF16),
                pltpu.VMEM((n_var, tile, LANES), F32),
                pltpu.VMEM((n_var, SUB, LANES), F32),
                pltpu.VMEM((2 * tile, CHUNK), BF16),
                pltpu.VMEM((n_layers + 1, tile, CHUNK), BF16),
                pltpu.VMEM((n_layers, tile, CHUNK), F32),
                pltpu.VMEM((n_layers, tile, CHUNK), F32),
                pltpu.VMEM((n_layers, width // 2 * SUB, CHUNK), BF16),
                pltpu.VMEM((tok_rows, c_token), F32),
                pltpu.VMEM((SUB, c_token), F32),
                pltpu.VMEM((n_steps, tok_rows, c_token), F32),
                pltpu.VMEM((n_steps, n_blocks, 6, tok_rows, c_token), F32),
                pltpu.VMEM((tok_rows, c_token), F32),
                pltpu.VMEM((n_dim, tok_rows), F32),
                pltpu.VMEM((n_rounds, n_peers, tok_rows, c_token), BF16),
                pltpu.SemaphoreType.DMA,
                pltpu.SemaphoreType.DMA((n_rounds, n_peers - 1)),
                pltpu.SemaphoreType.DMA((n_rounds, n_peers - 1)),
            ],
            compiler_params=pltpu.CompilerParams(collective_id=0, has_side_effects=True, vmem_limit_bytes=60 * 1024 * 1024),
            name="sampler",
        )(*ops)
        return swap(out)

    in_specs = (P("tok", None), P("tok", None), P("tok", None, None), P(part_axes, None), P(None, part_axes, None)) + (P(),) * 21
    return jax.shard_map(local_run, mesh=mesh, in_specs=in_specs, out_specs=P(part_axes, None), check_vma=False)
```

```python
import functools
import math
import jax
import jax.numpy as jnp
from jax import lax
from jax.experimental import pallas as pl
from jax.experimental.pallas import tpu as pltpu
from jax.sharding import PartitionSpec as P

SIGMA_DATA = 16.0
GAMMA = 0.8
NOISE_SCALE = 1.003
STEP_SCALE = 1.5
MASK_VALUE = -1e9
EPS = 1e-5
LOG2E = math.log2(math.e)
LANES = 128
SUB = 8
CHUNK = 256
UNROLL = 7
GROUPS = ((0,), (2, 1, 3))
F32 = jnp.float32
BF16 = jnp.bfloat16


def dot(a, b):
    return jnp.dot(a, b, preferred_element_type=F32)


def dot_t(a, b):
    return lax.dot_general(a, b, (((1,), (1,)), ((), ())), preferred_element_type=F32)


def spread(n):
    rows = lax.broadcasted_iota(jnp.int32, (n * SUB, n), 0)
    cols = lax.broadcasted_iota(jnp.int32, (n * SUB, n), 1)
    return (rows // SUB == cols).astype(BF16)


def expand_tall(tall):
    full = dot_t(tall.astype(BF16), spread(tall.shape[1]))
    rows = lax.broadcasted_iota(jnp.int32, full.shape, 0) & (SUB - 1)
    cols = lax.broadcasted_iota(jnp.int32, full.shape, 1) & (SUB - 1)
    return jnp.where(rows == cols, full, 0.0)


def expand(weight):
    return expand_tall(dot(spread(weight.shape[0]), weight)).astype(BF16)


def norm_major(values):
    parts = values.reshape(values.shape[0] // SUB, SUB, values.shape[1])
    inv = 1.0 / parts.shape[0]
    centered = parts - jnp.sum(parts, axis=0, keepdims=True) * inv
    variance = jnp.sum(centered * centered, axis=0, keepdims=True) * inv
    return (centered * lax.rsqrt(variance + EPS)).reshape(values.shape).astype(BF16)


def dot_tn(a, b):
    return lax.dot_general(a, b, (((0,), (0,)), ((), ())), preferred_element_type=F32)


def norm_cols(values):
    inv = 1.0 / values.shape[0]
    centered = values - jnp.sum(values, axis=0, keepdims=True) * inv
    variance = jnp.sum(centered * centered, axis=0, keepdims=True) * inv
    return centered * lax.rsqrt(variance + EPS)


def norm_rows(values):
    inv = 1.0 / values.shape[-1]
    centered = values - jnp.sum(values, axis=-1, keepdims=True) * inv
    variance = jnp.sum(centered * centered, axis=-1, keepdims=True) * inv
    return centered * lax.rsqrt(variance + EPS)


def sigmoid(h):
    return 0.5 + 0.5 * jnp.tanh(0.5 * h)


def silu(h):
    half = 0.5 * h
    return half + half * jnp.tanh(half)


def kernel(
    axis, n_peers,
    sig_ref, z_hbm, rel_ref, pin_ref, zup_ref, zdown_ref, pb_ref,
    st_ref, si_ref, x_ref, noise_ref, wsingle_ref, fw_ref, fb_ref, wfour_ref, wsup_ref, wsdown_ref,
    win_ref, wstok_ref, wcond_ref, gbias_ref, wqkvg_ref, wao_ref, wup_ref, wdown_ref, wout_ref,
    out_ref,
    z_s, bias_s, pwin_s, pwup_s, pwdown_s, pwpb_s, perm_s, rel_s, relsum_s,
    zn_s, xn_ss, cond_ss, held_ss, act_ss,
    bias_ts, wqkvg_ts, wao_ts, wup_ts, wdown_ts, cols_s, win_s, e_s, vt_s,
    base_s, four_s, astok_s, gate_s, acts_s, xs_s, y_s,
    z_sem, send_sem, recv_sem,
):
    me = lax.axis_index(axis)
    tok_rows, c_pair, n_tok = z_hbm.shape
    n_layers = zup_ref.shape[0]
    n_bins = rel_ref.shape[1]
    clip = (n_bins - 1) // 2
    n_blocks, n_heads = pb_ref.shape[0], pb_ref.shape[1]
    c_token = st_ref.shape[1]
    head_dim = c_token // n_heads
    n_steps = noise_ref.shape[0]
    n_valid = n_tok - tok_rows // 4
    tile = c_pair * SUB
    n_var = rel_s.shape[0]
    low = (clip + SUB) // SUB

    first = SUB * pl.cdiv(2 + 2 * n_layers, n_tok // CHUNK)
    z_parts = [pl.ds(0, first), pl.ds(first, tok_rows - first)]
    z_copies = [pltpu.make_async_copy(z_hbm.at[part], z_s.at[part], z_sem.at[i]) for i, part in enumerate(z_parts)]
    for copy in z_copies:
        copy.start()
    barrier = pltpu.get_barrier_semaphore()
    for off in range(1, n_peers):
        pl.semaphore_signal(barrier, inc=1, device_id={axis: lax.rem(me + off, n_peers)}, device_id_type=pl.DeviceIdType.MESH)

    row = lax.broadcasted_iota(jnp.int32, (SUB, 1), 0)
    t_col = jnp.full((SUB, 1), sig_ref[0] * (1.0 + GAMMA), F32)
    for k in range(1, n_steps):
        t_col = jnp.where(row == k, sig_ref[k] * (1.0 + GAMMA), t_col)
    level = 0.25 * jnp.log(t_col / SIGMA_DATA)
    feat = jnp.cos(2.0 * math.pi * (level * fw_ref[...] + fb_ref[...]))
    four_s[...] = lax.dot_general(wfour_ref[...], norm_rows(feat).astype(BF16), (((0,), (1,)), ((), ())), preferred_element_type=F32)
    joined = norm_rows(jnp.concatenate([st_ref[...].astype(F32), si_ref[...].astype(F32)], axis=-1)).astype(BF16)
    base_s[...] = lax.dot_general(wsingle_ref[...], joined, (((0,), (1,)), ((), ())), preferred_element_type=F32)
    n_dim = x_ref.shape[0]
    small = [gbias_ref[b] for b in range(n_blocks)] + [win_ref[...]]
    n_small = 2 * n_blocks + n_dim
    cols = jnp.transpose(jnp.concatenate(small + [jnp.zeros((-n_small % SUB, c_token), F32)], axis=0))
    cols_s[...] = cols
    for d in range(n_dim):
        win_s[d] = jnp.broadcast_to(cols[:, 2 * n_blocks + d:2 * n_blocks + d + 1], (c_token, tok_rows))

    def condition(k):
        single = base_s[...] + four_s[:, k:k + 1]
        for layer in range(wsup_ref.shape[0]):
            h = dot_tn(wsup_ref[layer], norm_cols(single).astype(BF16))
            half = h.shape[0] // 2
            act = (silu(h[:half]) * h[half:]).astype(BF16)
            single = single + dot_tn(wsdown_ref[layer], act)
        u = norm_cols(single).astype(BF16)
        astok_s[k] = dot_tn(wstok_ref[...], u)
        for b in range(n_blocks):
            cond = dot_tn(wcond_ref[b], u)
            part = lambda i: cond[i * c_token:(i + 1) * c_token]
            gate_s[k, b, 0] = sigmoid(part(0))
            gate_s[k, b, 1] = part(1)
            gate_s[k, b, 2] = sigmoid(part(2) + cols_s[:, 2 * b:2 * b + 1])
            gate_s[k, b, 3] = sigmoid(part(3))
            gate_s[k, b, 4] = part(4)
            gate_s[k, b, 5] = sigmoid(part(5) + cols_s[:, 2 * b + 1:2 * b + 2])

    def copies(r):
        out = []
        for off in sorted(range(1, n_peers), key=lambda o: -min(o, n_peers - o)):
            peer = lax.rem(me + off, n_peers)
            out.append(pltpu.make_async_remote_copy(
                src_ref=y_s.at[r, me], dst_ref=y_s.at[r, me],
                send_sem=send_sem.at[r, off], recv_sem=recv_sem.at[r, me],
                device_id={axis: peer}, device_id_type=pl.DeviceIdType.MESH))
        return out

    def wait_from(r, src):
        pltpu.make_async_remote_copy(
            src_ref=y_s.at[r, src], dst_ref=y_s.at[r, src],
            send_sem=send_sem.at[r, 0], recv_sem=recv_sem.at[r, src],
            device_id={axis: src}, device_id_type=pl.DeviceIdType.MESH).wait_recv()

    def noisy(k):
        c = jnp.full((1, tok_rows), sig_ref[k], F32)
        t = c * (1.0 + GAMMA)
        xn = xs_s[...] + NOISE_SCALE * jnp.sqrt(t * t - c * c) * noise_ref[k]
        return xn, t, t * t + SIGMA_DATA * SIGMA_DATA

    def begin(k):
        xn, t, var = noisy(k)
        r = xn / jnp.sqrt(var)
        lin = r[0:1] * win_s[0]
        for d in range(1, n_dim):
            lin = lin + r[d:d + 1] * win_s[d]
        acts_s[...] = lin + astok_s[k]

    def pack(k, b, r):
        y_s[r, me] = (gate_s[k, b, 0] * norm_cols(acts_s[...]) + gate_s[k, b, 1]).astype(BF16)

    def send(r):
        for copy in copies(r):
            copy.start()

    pin = pin_ref[...]
    pwin_s[:, :tile] = expand(pin[:, :c_pair])
    pwin_s[:, tile:] = expand(pin[:, c_pair:])
    for layer in range(n_layers):
        up = zup_ref[layer]
        width = up.shape[1]
        full = expand_tall(dot_t(spread(width), up))
        gate_rows = lax.broadcasted_iota(jnp.int32, full.shape, 0) < (width // 2) * SUB
        pwup_s[layer] = jnp.where(gate_rows, 0.5 * full, full).astype(BF16)
        pwdown_s[layer] = expand(zdown_ref[layer])
    for b in range(n_blocks):
        pwpb_s[b * n_heads * SUB:(b + 1) * n_heads * SUB, :] = expand(pb_ref[b])
    rows_i = lax.broadcasted_iota(jnp.int32, (tile, tile), 0)
    cols_i = lax.broadcasted_iota(jnp.int32, (tile, tile), 1)
    perm_s[...] = ((rows_i & (SUB - 1)) * c_pair + rows_i // SUB == cols_i).astype(BF16)
    tall = dot(spread(c_pair), rel_ref[...]).astype(BF16)
    bin_i = lax.broadcasted_iota(jnp.int32, (n_bins, LANES), 0)
    diag_i = lax.broadcasted_iota(jnp.int32, (n_bins, LANES), 1)
    row_s = lax.broadcasted_iota(jnp.int32, (tile, LANES), 0) & (SUB - 1)
    tab = jnp.zeros((tile, LANES), F32)
    for s in range(SUB):
        pick = (bin_i == jnp.clip(diag_i - (SUB - 1) + s, 0, n_bins - 1)).astype(BF16)
        tab = jnp.where(row_s == s, dot(tall, pick), tab)
    tab = tab.astype(BF16)

    per = 2
    k_i = lax.broadcasted_iota(jnp.int32, (LANES, LANES), 0)
    j_i = lax.broadcasted_iota(jnp.int32, (LANES, LANES), 1)

    for i in range(0, n_var, per):
        picks = []
        for v in range(i, i + per):
            want = jnp.clip(SUB * (v - low) - j_i + clip + SUB - 1, 0, n_bins + SUB - 2)
            picks.append((k_i == want).astype(BF16))
        planes = dot(tab, jnp.concatenate(picks, axis=1))
        for v in range(i, i + per):
            plane = planes[:, (v - i) * LANES:(v - i + 1) * LANES]
            rel_s[v] = plane
            relsum_s[v] = jnp.sum(plane.reshape(c_pair, SUB, LANES), axis=0)

    n_chunks = n_tok // CHUNK
    total = (tok_rows // SUB) * n_chunks
    depth = 2 + 2 * n_layers

    def trip(it):
        known = isinstance(it, int)

        def active(lag):
            return not known or 0 <= it - lag < total

        def place(lag):
            idx = it - lag
            r0, c0 = (idx // n_chunks) * SUB, (idx % n_chunks) * CHUNK
            return (r0, c0) if known else (pl.multiple_of(r0, SUB), pl.multiple_of(c0, CHUNK))

        if active(depth):
            r0, c0 = place(depth)
            bias = dot(pwpb_s[...], xn_ss[n_layers])
            bias = bias.astype(BF16).astype(F32) * LOG2E
            bias_s[:, pl.ds(r0, SUB), pl.ds(c0, CHUNK)] = bias.reshape(n_blocks * n_heads, SUB, CHUNK)
        for layer in reversed(range(n_layers)):
            if active(3 + 2 * layer):
                cond = held_ss[layer] + dot(pwdown_s[layer], act_ss[layer])
                xn_ss[layer + 1] = norm_major(cond)
            if active(2 + 2 * layer):
                h = dot(pwup_s[layer], xn_ss[layer])
                half = h.shape[0] // 2
                gate = h[:half]
                act_ss[layer] = ((gate + gate * jnp.tanh(gate)) * h[half:]).astype(BF16)
                held_ss[layer] = cond_ss[layer]
            if active(3 + 2 * layer) and layer + 1 < n_layers:
                cond_ss[layer + 1] = cond
        if active(1):
            cond = dot(pwin_s[...], zn_s[...])
            cond_ss[0] = cond
            xn_ss[0] = norm_major(cond)
        if active(0):
            r0, c0 = place(0)
            zb = z_s[pl.ds(r0, SUB), :, pl.ds(c0, CHUNK)].reshape(tile, CHUNK)
            z = dot(perm_s[...], zb).reshape(c_pair, SUB, CHUNK)
            rels, sums = [], []
            for part in range(CHUNK // LANES):
                delta = me * tok_rows + r0 - c0 - part * LANES
                v = jnp.clip(delta // SUB + low, 0, n_var - 1)
                rels.append(rel_s[v])
                sums.append(relsum_s[v])
            rel = jnp.concatenate(rels, axis=1).reshape(c_pair, SUB, CHUNK)
            inv = 1.0 / (2 * c_pair)
            mean = (jnp.sum(z, axis=0) + jnp.concatenate(sums, axis=1)) * inv
            zc = z - mean
            rc = rel - mean
            var = (jnp.sum(zc * zc, axis=0) + jnp.sum(rc * rc, axis=0)) * inv
            rs = lax.rsqrt(var + EPS)
            zn_s[:tile] = (zc * rs).reshape(tile, CHUNK).astype(BF16)
            zn_s[tile:] = (rc * rs).reshape(tile, CHUNK).astype(BF16)

    loops = (total - depth) // UNROLL

    def trips(i, carry):
        for j in range(UNROLL):
            trip(depth + i * UNROLL + j)
        return carry

    for b in range(n_blocks):
        wqkvg_ts[b] = jnp.transpose(wqkvg_ref[b])
        wao_ts[b] = jnp.transpose(wao_ref[b])
        wup_ts[b] = jnp.transpose(wup_ref[b])
        wdown_ts[b] = jnp.transpose(wdown_ref[b])
    z_copies[0].wait()
    condition(0)
    xs_s[...] = sig_ref[0] * x_ref[...]
    begin(0)
    for it in range(depth):
        trip(it)
    pack(0, 0, 0)
    pl.semaphore_wait(barrier, n_peers - 1)
    send(0)
    z_copies[1].wait()
    lax.fori_loop(0, loops, trips, 0)
    for it in range(depth + loops * UNROLL, total + depth):
        trip(it)

    def turn(b):
        for h in range(n_heads):
            for key0 in range(0, n_tok, LANES):
                bias_ts[b, key0:key0 + LANES, h * tok_rows:(h + 1) * tok_rows] = jnp.transpose(bias_s[b * n_heads + h, :, key0:key0 + LANES])

    head = lax.broadcasted_iota(jnp.int32, (c_token, 1), 0) // head_dim
    scale = head_dim ** -0.5 * LOG2E
    cores = 2
    n_chips = n_peers // cores
    chip_keys = cores * tok_rows
    my_chip = me // cores

    def block(k, b):
        r = k * n_blocks + b
        y = y_s[r, me]
        q = dot(wqkvg_ts[b, :c_token, :], y)
        g = sigmoid(dot(wqkvg_ts[b, 3 * c_token:, :], y))
        q_heads = jnp.concatenate([jnp.where(head == h, q, 0.0).astype(BF16) for h in range(n_heads)], axis=1)
        tops, sums = [], []
        pos = 0
        for group in GROUPS:
            chips = [lax.rem(my_chip + d, n_chips) for d in group]
            for d, chip in zip(group, chips):
                if d == 0:
                    wait_from(r, me + 1 - 2 * lax.rem(me, cores))
                else:
                    for c in range(cores):
                        wait_from(r, chip * cores + c)
            y_group = jnp.concatenate([y_s[r, chip * cores + c] for chip in chips for c in range(cores)], axis=1)
            kv = dot(wqkvg_ts[b, c_token:3 * c_token, :], y_group).astype(BF16)
            vt_s[:, pos * chip_keys:(pos + len(group)) * chip_keys] = kv[c_token:]
            scores = dot_tn(kv[:c_token], q_heads)
            for i, chip in enumerate(chips):
                key0 = pl.multiple_of(chip * chip_keys, chip_keys)
                sc = scores[i * chip_keys:(i + 1) * chip_keys] * scale + bias_ts[b, pl.ds(key0, chip_keys), :]
                key_ok = lax.broadcasted_iota(jnp.int32, (chip_keys, 1), 0) + key0 < n_valid
                sc = jnp.where(key_ok, sc, MASK_VALUE * LOG2E)
                top = jnp.max(sc, axis=0, keepdims=True)
                e = jnp.exp2(sc - top)
                e_s[pos] = e
                tops.append(top)
                sums.append(jnp.sum(e, axis=0, keepdims=True))
                pos += 1
        best = functools.reduce(jnp.maximum, tops)
        scales = [jnp.exp2(top - best) for top in tops]
        inv = 1.0 / functools.reduce(jnp.add, [f * l for f, l in zip(scales, sums)])
        probs = jnp.concatenate([(e_s[i] * (scales[i] * inv)).astype(BF16) for i in range(pos)], axis=0)
        mix = []
        for h in range(0, n_heads, 2):
            pair = dot(vt_s[h * head_dim:(h + 2) * head_dim, :], probs[:, h * tok_rows:(h + 2) * tok_rows])
            mix += [pair[:head_dim, :tok_rows], pair[head_dim:, tok_rows:]]
        attn = dot(wao_ts[b], (g * jnp.concatenate(mix, axis=0)).astype(BF16))
        acts = acts_s[...] + gate_s[k, b, 2] * attn
        normed = (gate_s[k, b, 3] * norm_cols(acts) + gate_s[k, b, 4]).astype(BF16)
        h = dot(wup_ts[b], normed)
        half = h.shape[0] // 2
        act = (silu(h[:half]) * h[half:]).astype(BF16)
        acts_s[...] = acts + gate_s[k, b, 5] * dot(wdown_ts[b], act)
        for copy in copies(r):
            copy.wait_send()

    turn(0)

    def step(k, carry):
        @pl.when(k > 0)
        def _():
            begin(k)
            pack(k, 0, k * n_blocks)
            send(k * n_blocks)

        block(k, 0)
        for b in range(1, n_blocks):
            pack(k, b, k * n_blocks + b)
            send(k * n_blocks + b)

            @pl.when(k == 0)
            def _():
                turn(b)
                if b == 1:
                    for later in range(1, n_steps):
                        condition(later)

            block(k, b)
        xn, t, var = noisy(k)
        update = dot(wout_ref[...], norm_cols(acts_s[...]).astype(BF16))
        denoised = (SIGMA_DATA * SIGMA_DATA / var) * xn + (t * SIGMA_DATA / jnp.sqrt(var)) * update
        xs_s[...] = xn + STEP_SCALE * (sig_ref[k + 1] - t) * (xn - denoised) / t
        return carry

    lax.fori_loop(0, n_steps, step, 0)
    out_ref[...] = xs_s[...]


def solution(mesh):
    part_axes = ("sample", "tok")
    n_peers = mesh.shape["tok"]

    def local_run(s_trunk, s_inputs, z_trunk, x_noise, step_noise, sigmas, relpos_table, w_pair_in, w_z_up, w_z_down, w_pair_bias, w_single, fourier_w, fourier_b, w_fourier, w_s_up, w_s_down, w_in, w_s_tok, w_cond, gate_bias, w_qkvg, w_attn_out, w_up, w_down, w_out):
        tok_rows, n_tok, c_pair = z_trunk.shape
        n_steps, _, n_dim = step_noise.shape
        n_blocks, _, n_heads = w_pair_bias.shape
        n_layers, _, width = w_z_up.shape
        c_token = w_qkvg.shape[1]
        clip = (relpos_table.shape[0] - 1) // 2
        tile = c_pair * SUB
        n_var = 2 * clip // SUB + LANES // SUB + 2
        n_rounds = n_steps * n_blocks
        swap = lambda a: jnp.swapaxes(a, -1, -2)
        ops = [
            sigmas, swap(z_trunk), swap(relpos_table), swap(w_pair_in), w_z_up, swap(w_z_down), swap(w_pair_bias),
            s_trunk, s_inputs, swap(x_noise), swap(step_noise), w_single, fourier_w[None, :], fourier_b[None, :], w_fourier, w_s_up, w_s_down,
            w_in, w_s_tok, w_cond, gate_bias, w_qkvg, w_attn_out, w_up, w_down, swap(w_out),
        ]
        specs = [pl.BlockSpec(memory_space=pltpu.SMEM), pl.BlockSpec(memory_space=pl.ANY)] + [pl.BlockSpec(memory_space=pltpu.VMEM)] * (len(ops) - 2)
        out = pl.pallas_call(
            functools.partial(kernel, "tok", n_peers),
            in_specs=specs,
            out_specs=pl.BlockSpec(memory_space=pltpu.VMEM),
            out_shape=jax.ShapeDtypeStruct((n_dim, tok_rows), F32),
            scratch_shapes=[
                pltpu.VMEM((tok_rows, c_pair, n_tok), BF16),
                pltpu.VMEM((n_blocks * n_heads, tok_rows, n_tok), F32),
                pltpu.VMEM((tile, 2 * tile), BF16),
                pltpu.VMEM((n_layers, width * SUB, tile), BF16),
                pltpu.VMEM((n_layers, tile, width // 2 * SUB), BF16),
                pltpu.VMEM((n_blocks * n_heads * SUB, tile), BF16),
                pltpu.VMEM((tile, tile), BF16),
                pltpu.VMEM((n_var, tile, LANES), F32),
                pltpu.VMEM((n_var, SUB, LANES), F32),
                pltpu.VMEM((2 * tile, CHUNK), BF16),
                pltpu.VMEM((n_layers + 1, tile, CHUNK), BF16),
                pltpu.VMEM((n_layers, tile, CHUNK), F32),
                pltpu.VMEM((n_layers, tile, CHUNK), F32),
                pltpu.VMEM((n_layers, width // 2 * SUB, CHUNK), BF16),
                pltpu.VMEM((n_blocks, n_tok, n_heads * tok_rows), F32),
                pltpu.VMEM((n_blocks, 4 * c_token, c_token), BF16),
                pltpu.VMEM((n_blocks, c_token, c_token), BF16),
                pltpu.VMEM((n_blocks, w_up.shape[2], c_token), BF16),
                pltpu.VMEM((n_blocks, c_token, w_down.shape[1]), BF16),
                pltpu.VMEM((c_token, SUB), F32),
                pltpu.VMEM((n_dim, c_token, tok_rows), F32),
                pltpu.VMEM((n_peers // 2, 2 * tok_rows, n_heads * tok_rows), F32),
                pltpu.VMEM((c_token, n_tok), BF16),
                pltpu.VMEM((c_token, tok_rows), F32),
                pltpu.VMEM((c_token, SUB), F32),
                pltpu.VMEM((n_steps, c_token, tok_rows), F32),
                pltpu.VMEM((n_steps, n_blocks, 6, c_token, tok_rows), F32),
                pltpu.VMEM((c_token, tok_rows), F32),
                pltpu.VMEM((n_dim, tok_rows), F32),
                pltpu.VMEM((n_rounds, n_peers, c_token, tok_rows), BF16),
                pltpu.SemaphoreType.DMA((2,)),
                pltpu.SemaphoreType.DMA((n_rounds, n_peers)),
                pltpu.SemaphoreType.DMA((n_rounds, n_peers)),
            ],
            compiler_params=pltpu.CompilerParams(collective_id=0, has_side_effects=True, vmem_limit_bytes=60 * 1024 * 1024),
            name="sampler",
        )(*ops)
        return swap(out)

    in_specs = (P("tok", None), P("tok", None), P("tok", None, None), P(part_axes, None), P(None, part_axes, None)) + (P(),) * 21
    return jax.shard_map(local_run, mesh=mesh, in_specs=in_specs, out_specs=P(part_axes, None), check_vma=False)
```

```python
import functools
import math
import jax
import jax.numpy as jnp
from jax import lax
from jax.experimental import pallas as pl
from jax.experimental.pallas import tpu as pltpu
from jax.sharding import PartitionSpec as P

SIGMA_DATA = 16.0
GAMMA = 0.8
NOISE_SCALE = 1.003
STEP_SCALE = 1.5
MASK_VALUE = -1e9
EPS = 1e-5
LOG2E = math.log2(math.e)
LANES = 128
SUB = 8
CHUNK = 256
UNROLL = 7
GROUPS = ((0,), (2, 1, 3))
F32 = jnp.float32
BF16 = jnp.bfloat16


def dot(a, b):
    return jnp.dot(a, b, preferred_element_type=F32)


def dot_t(a, b):
    return lax.dot_general(a, b, (((1,), (1,)), ((), ())), preferred_element_type=F32)


def spread(n):
    rows = lax.broadcasted_iota(jnp.int32, (n * SUB, n), 0)
    cols = lax.broadcasted_iota(jnp.int32, (n * SUB, n), 1)
    return (rows // SUB == cols).astype(BF16)


def expand_tall(tall):
    full = dot_t(tall.astype(BF16), spread(tall.shape[1]))
    rows = lax.broadcasted_iota(jnp.int32, full.shape, 0) & (SUB - 1)
    cols = lax.broadcasted_iota(jnp.int32, full.shape, 1) & (SUB - 1)
    return jnp.where(rows == cols, full, 0.0)


def expand(weight):
    return expand_tall(dot(spread(weight.shape[0]), weight)).astype(BF16)


def norm_major(values):
    parts = values.reshape(values.shape[0] // SUB, SUB, values.shape[1])
    inv = 1.0 / parts.shape[0]
    centered = parts - jnp.sum(parts, axis=0, keepdims=True) * inv
    variance = jnp.sum(centered * centered, axis=0, keepdims=True) * inv
    return (centered * lax.rsqrt(variance + EPS)).reshape(values.shape).astype(BF16)


def dot_tn(a, b):
    return lax.dot_general(a, b, (((0,), (0,)), ((), ())), preferred_element_type=F32)


def norm_cols(values):
    inv = 1.0 / values.shape[0]
    centered = values - jnp.sum(values, axis=0, keepdims=True) * inv
    variance = jnp.sum(centered * centered, axis=0, keepdims=True) * inv
    return centered * lax.rsqrt(variance + EPS)


def norm_rows(values):
    inv = 1.0 / values.shape[-1]
    centered = values - jnp.sum(values, axis=-1, keepdims=True) * inv
    variance = jnp.sum(centered * centered, axis=-1, keepdims=True) * inv
    return centered * lax.rsqrt(variance + EPS)


def sigmoid(h):
    return 0.5 + 0.5 * jnp.tanh(0.5 * h)


def silu(h):
    half = 0.5 * h
    return half + half * jnp.tanh(half)


def kernel(
    axis, n_peers,
    sig_ref, z_hbm, rel_ref, pin_ref, zup_ref, zdown_ref, pb_ref,
    st_ref, si_ref, x_ref, noise_ref, wsingle_ref, fw_ref, fb_ref, wfour_ref, wsup_ref, wsdown_ref,
    win_ref, wstok_ref, wcond_ref, gbias_ref, wqkvg_ref, wao_ref, wup_ref, wdown_ref, wout_ref,
    out_ref,
    z_s, bias_s, pwin_s, pwup_s, pwdown_s, pwpb_s, perm_s, rel_s, relsum_s,
    zn_s, xn_ss, cond_ss, held_ss, act_ss,
    bias_ts, wqkvg_ts, wao_ts, wup_ts, wdown_ts, cols_s, win_s, e_s, vt_s,
    base_s, four_s, astok_s, gate_s, acts_s, xs_s, y_s, u_own, u_s, r_s, ast_all, mul_all, add_all,
    z_sem, y_send, y_recv, u_send, u_recv, r_send, r_recv,
):
    me = lax.axis_index(axis)
    tok_rows, c_pair, n_tok = z_hbm.shape
    n_layers = zup_ref.shape[0]
    n_bins = rel_ref.shape[1]
    clip = (n_bins - 1) // 2
    n_blocks, n_heads = pb_ref.shape[0], pb_ref.shape[1]
    c_token = st_ref.shape[1]
    head_dim = c_token // n_heads
    n_steps = noise_ref.shape[0]
    n_valid = n_tok - tok_rows // 4
    tile = c_pair * SUB
    n_var = rel_s.shape[0]
    low = (clip + SUB) // SUB

    first = SUB * pl.cdiv(2 + 2 * n_layers, n_tok // CHUNK)
    z_parts = [pl.ds(0, first), pl.ds(first, tok_rows - first)]
    z_copies = [pltpu.make_async_copy(z_hbm.at[part], z_s.at[part], z_sem.at[i]) for i, part in enumerate(z_parts)]
    for copy in z_copies:
        copy.start()
    barrier = pltpu.get_barrier_semaphore()
    for off in range(1, n_peers):
        pl.semaphore_signal(barrier, inc=1, device_id={axis: lax.rem(me + off, n_peers)}, device_id_type=pl.DeviceIdType.MESH)

    row = lax.broadcasted_iota(jnp.int32, (SUB, 1), 0)
    t_col = jnp.full((SUB, 1), sig_ref[0] * (1.0 + GAMMA), F32)
    for k in range(1, n_steps):
        t_col = jnp.where(row == k, sig_ref[k] * (1.0 + GAMMA), t_col)
    level = 0.25 * jnp.log(t_col / SIGMA_DATA)
    feat = jnp.cos(2.0 * math.pi * (level * fw_ref[...] + fb_ref[...]))
    four_s[...] = lax.dot_general(wfour_ref[...], norm_rows(feat).astype(BF16), (((0,), (1,)), ((), ())), preferred_element_type=F32)
    joined = norm_rows(jnp.concatenate([st_ref[...].astype(F32), si_ref[...].astype(F32)], axis=-1)).astype(BF16)
    base_s[...] = lax.dot_general(wsingle_ref[...], joined, (((0,), (1,)), ((), ())), preferred_element_type=F32)
    n_dim = x_ref.shape[0]
    small = [gbias_ref[b] for b in range(n_blocks)] + [win_ref[...]]
    n_small = 2 * n_blocks + n_dim
    cols = jnp.transpose(jnp.concatenate(small + [jnp.zeros((-n_small % SUB, c_token), F32)], axis=0))
    cols_s[...] = cols
    for d in range(n_dim):
        win_s[d] = jnp.broadcast_to(cols[:, 2 * n_blocks + d:2 * n_blocks + d + 1], (c_token, tok_rows))

    def condition():
        single = jnp.concatenate([base_s[...] + four_s[:, k:k + 1] for k in range(n_steps)], axis=1)
        for layer in range(wsup_ref.shape[0]):
            h = dot_tn(wsup_ref[layer], norm_cols(single).astype(BF16))
            half = h.shape[0] // 2
            act = (silu(h[:half]) * h[half:]).astype(BF16)
            single = single + dot_tn(wsdown_ref[layer], act)
        u = norm_cols(single).astype(BF16)
        for k in range(n_steps):
            u_own[k] = u[:, k * tok_rows:(k + 1) * tok_rows]

    def gates(first, last):
        u = jnp.concatenate([u_own[k] for k in range(first, last)], axis=1)
        acts = dot_tn(wstok_ref[...], u)
        at = lambda v, k: v[:, (k - first) * tok_rows:(k - first + 1) * tok_rows]
        for k in range(first, last):
            astok_s[k] = at(acts, k)
        for b in range(n_blocks):
            cond = dot_tn(wcond_ref[b], u)
            part = lambda i: cond[i * c_token:(i + 1) * c_token]
            rows = [sigmoid(part(0)), part(1), sigmoid(part(2) + cols_s[:, 2 * b:2 * b + 1]), sigmoid(part(3)), part(4), sigmoid(part(5) + cols_s[:, 2 * b + 1:2 * b + 2])]
            for i, gate in enumerate(rows):
                for k in range(first, last):
                    gate_s[k, b, i] = at(gate, k)

    def copies(buf, i, send_sem, recv_sem):
        out = []
        for off in sorted(range(1, n_peers), key=lambda o: -min(o, n_peers - o)):
            peer = lax.rem(me + off, n_peers)
            out.append(pltpu.make_async_remote_copy(
                src_ref=buf.at[i, me], dst_ref=buf.at[i, me],
                send_sem=send_sem.at[i, off], recv_sem=recv_sem.at[i, me],
                device_id={axis: peer}, device_id_type=pl.DeviceIdType.MESH))
        return out

    def wait_from(buf, i, send_sem, recv_sem, src):
        pltpu.make_async_remote_copy(
            src_ref=buf.at[i, src], dst_ref=buf.at[i, src],
            send_sem=send_sem.at[i, 0], recv_sem=recv_sem.at[i, src],
            device_id={axis: src}, device_id_type=pl.DeviceIdType.MESH).wait_recv()

    y_set = (y_send, y_recv)
    u_set = (u_send, u_recv)
    r_set = (r_send, r_recv)

    def noisy(k):
        c = jnp.full((1, tok_rows), sig_ref[k], F32)
        t = c * (1.0 + GAMMA)
        xn = xs_s[...] + NOISE_SCALE * jnp.sqrt(t * t - c * c) * noise_ref[k]
        return xn, t, t * t + SIGMA_DATA * SIGMA_DATA

    def begin(k):
        xn, t, var = noisy(k)
        r = xn / jnp.sqrt(var)
        lin = r[0:1] * win_s[0]
        for d in range(1, n_dim):
            lin = lin + r[d:d + 1] * win_s[d]
        acts_s[...] = lin + astok_s[k]
        return r

    def pack(k, b):
        return (gate_s[k, b, 0] * norm_cols(acts_s[...]) + gate_s[k, b, 1]).astype(BF16)

    pin = pin_ref[...]
    pwin_s[:, :tile] = expand(pin[:, :c_pair])
    pwin_s[:, tile:] = expand(pin[:, c_pair:])
    for layer in range(n_layers):
        up = zup_ref[layer]
        width = up.shape[1]
        full = expand_tall(dot_t(spread(width), up))
        gate_rows = lax.broadcasted_iota(jnp.int32, full.shape, 0) < (width // 2) * SUB
        pwup_s[layer] = jnp.where(gate_rows, 0.5 * full, full).astype(BF16)
        pwdown_s[layer] = expand(zdown_ref[layer])
    for b in range(n_blocks):
        pwpb_s[b * n_heads * SUB:(b + 1) * n_heads * SUB, :] = expand(pb_ref[b])
    rows_i = lax.broadcasted_iota(jnp.int32, (tile, tile), 0)
    cols_i = lax.broadcasted_iota(jnp.int32, (tile, tile), 1)
    perm_s[...] = ((rows_i & (SUB - 1)) * c_pair + rows_i // SUB == cols_i).astype(BF16)
    tall = dot(spread(c_pair), rel_ref[...]).astype(BF16)
    bin_i = lax.broadcasted_iota(jnp.int32, (n_bins, LANES), 0)
    diag_i = lax.broadcasted_iota(jnp.int32, (n_bins, LANES), 1)
    row_s = lax.broadcasted_iota(jnp.int32, (tile, LANES), 0) & (SUB - 1)
    tab = jnp.zeros((tile, LANES), F32)
    for s in range(SUB):
        pick = (bin_i == jnp.clip(diag_i - (SUB - 1) + s, 0, n_bins - 1)).astype(BF16)
        tab = jnp.where(row_s == s, dot(tall, pick), tab)
    tab = tab.astype(BF16)

    per = 2
    k_i = lax.broadcasted_iota(jnp.int32, (LANES, LANES), 0)
    j_i = lax.broadcasted_iota(jnp.int32, (LANES, LANES), 1)

    for i in range(0, n_var, per):
        picks = []
        for v in range(i, i + per):
            want = jnp.clip(SUB * (v - low) - j_i + clip + SUB - 1, 0, n_bins + SUB - 2)
            picks.append((k_i == want).astype(BF16))
        planes = dot(tab, jnp.concatenate(picks, axis=1))
        for v in range(i, i + per):
            plane = planes[:, (v - i) * LANES:(v - i + 1) * LANES]
            rel_s[v] = plane
            relsum_s[v] = jnp.sum(plane.reshape(c_pair, SUB, LANES), axis=0)

    n_chunks = n_tok // CHUNK
    total = (tok_rows // SUB) * n_chunks
    depth = 2 + 2 * n_layers

    def trip(it):
        known = isinstance(it, int)

        def active(lag):
            return not known or 0 <= it - lag < total

        def place(lag):
            idx = it - lag
            r0, c0 = (idx // n_chunks) * SUB, (idx % n_chunks) * CHUNK
            return (r0, c0) if known else (pl.multiple_of(r0, SUB), pl.multiple_of(c0, CHUNK))

        if active(depth):
            r0, c0 = place(depth)
            bias = dot(pwpb_s[...], xn_ss[n_layers])
            bias = bias.astype(BF16).astype(F32) * LOG2E
            bias_s[:, pl.ds(r0, SUB), pl.ds(c0, CHUNK)] = bias.reshape(n_blocks * n_heads, SUB, CHUNK)
        for layer in reversed(range(n_layers)):
            if active(3 + 2 * layer):
                cond = held_ss[layer] + dot(pwdown_s[layer], act_ss[layer])
                xn_ss[layer + 1] = norm_major(cond)
            if active(2 + 2 * layer):
                h = dot(pwup_s[layer], xn_ss[layer])
                half = h.shape[0] // 2
                gate = h[:half]
                act_ss[layer] = ((gate + gate * jnp.tanh(gate)) * h[half:]).astype(BF16)
                held_ss[layer] = cond_ss[layer]
            if active(3 + 2 * layer) and layer + 1 < n_layers:
                cond_ss[layer + 1] = cond
        if active(1):
            cond = dot(pwin_s[...], zn_s[...])
            cond_ss[0] = cond
            xn_ss[0] = norm_major(cond)
        if active(0):
            r0, c0 = place(0)
            zb = z_s[pl.ds(r0, SUB), :, pl.ds(c0, CHUNK)].reshape(tile, CHUNK)
            z = dot(perm_s[...], zb).reshape(c_pair, SUB, CHUNK)
            rels, sums = [], []
            for part in range(CHUNK // LANES):
                delta = me * tok_rows + r0 - c0 - part * LANES
                v = jnp.clip(delta // SUB + low, 0, n_var - 1)
                rels.append(rel_s[v])
                sums.append(relsum_s[v])
            rel = jnp.concatenate(rels, axis=1).reshape(c_pair, SUB, CHUNK)
            inv = 1.0 / (2 * c_pair)
            mean = (jnp.sum(z, axis=0) + jnp.concatenate(sums, axis=1)) * inv
            zc = z - mean
            rc = rel - mean
            var = (jnp.sum(zc * zc, axis=0) + jnp.sum(rc * rc, axis=0)) * inv
            rs = lax.rsqrt(var + EPS)
            zn_s[:tile] = (zc * rs).reshape(tile, CHUNK).astype(BF16)
            zn_s[tile:] = (rc * rs).reshape(tile, CHUNK).astype(BF16)

    loops = (total - depth) // UNROLL

    def trips(i, carry):
        for j in range(UNROLL):
            trip(depth + i * UNROLL + j)
        return carry

    for b in range(n_blocks):
        wqkvg_ts[b] = jnp.transpose(wqkvg_ref[b])
        wao_ts[b] = jnp.transpose(wao_ref[b])
        wup_ts[b] = jnp.transpose(wup_ref[b])
        wdown_ts[b] = jnp.transpose(wdown_ref[b])
    z_copies[0].wait()
    condition()
    gates(0, 1)
    xs_s[...] = sig_ref[0] * x_ref[...]
    begin(0)
    for it in range(depth):
        trip(it)
    y_s[0, me] = pack(0, 0)
    for k in range(1, n_steps):
        u_s[k, me] = u_own[k]
    pl.semaphore_wait(barrier, n_peers - 1)
    for copy in copies(y_s, 0, *y_set):
        copy.start()
    for k in range(1, n_steps):
        for copy in copies(u_s, k, *u_set):
            copy.start()
    z_copies[1].wait()
    lax.fori_loop(0, loops, trips, 0)
    for it in range(depth + loops * UNROLL, total + depth):
        trip(it)

    def turn(b):
        for h in range(n_heads):
            for key0 in range(0, n_tok, LANES):
                bias_ts[b, key0:key0 + LANES, h * tok_rows:(h + 1) * tok_rows] = jnp.transpose(bias_s[b * n_heads + h, :, key0:key0 + LANES])

    head = lax.broadcasted_iota(jnp.int32, (c_token, 1), 0) // head_dim
    scale = head_dim ** -0.5 * LOG2E
    cores = 2
    n_chips = n_peers // cores
    chip_keys = cores * tok_rows
    my_chip = me // cores

    def others(d, chip):
        return [me + 1 - 2 * lax.rem(me, cores)] if d == 0 else [chip * cores + c for c in range(cores)]

    def block(k, b):
        r = k * n_blocks + b
        rebuilt = k > 0 and b == 0
        y = pack(k, b) if rebuilt else y_s[r, me]
        q = dot(wqkvg_ts[b, :c_token, :], y)
        g = sigmoid(dot(wqkvg_ts[b, 3 * c_token:, :], y))
        q_heads = jnp.concatenate([jnp.where(head == h, q, 0.0).astype(BF16) for h in range(n_heads)], axis=1)
        tops, sums = [], []
        pos = 0
        for group in GROUPS if r > 0 else (sum(GROUPS, ()),):
            chips = [lax.rem(my_chip + d, n_chips) for d in group]
            for d, chip in zip(group, chips):
                for src in others(d, chip):
                    if rebuilt:
                        wait_from(r_s, k, *r_set, src)
                    else:
                        wait_from(y_s, r, *y_set, src)
            if rebuilt:
                parts = []
                for chip in chips:
                    keys = pl.ds(pl.multiple_of(chip * chip_keys, chip_keys), chip_keys)
                    pos_r = jnp.concatenate([r_s[k, chip * cores + c] for c in range(cores)], axis=1)
                    lin = pos_r[0:1] * jnp.concatenate([win_s[0]] * cores, axis=1)
                    for d in range(1, n_dim):
                        lin = lin + pos_r[d:d + 1] * jnp.concatenate([win_s[d]] * cores, axis=1)
                    parts.append((mul_all[:, keys] * norm_cols(lin + ast_all[:, keys]) + add_all[:, keys]).astype(BF16))
                y_group = jnp.concatenate(parts, axis=1)
            else:
                y_group = jnp.concatenate([y_s[r, chip * cores + c] for chip in chips for c in range(cores)], axis=1)
            kv = dot(wqkvg_ts[b, c_token:3 * c_token, :], y_group).astype(BF16)
            vt_s[:, pos * chip_keys:(pos + len(group)) * chip_keys] = kv[c_token:]
            scores = dot_tn(kv[:c_token], q_heads)
            for i, chip in enumerate(chips):
                key0 = pl.multiple_of(chip * chip_keys, chip_keys)
                sc = scores[i * chip_keys:(i + 1) * chip_keys] * scale + bias_ts[b, pl.ds(key0, chip_keys), :]
                key_ok = lax.broadcasted_iota(jnp.int32, (chip_keys, 1), 0) + key0 < n_valid
                sc = jnp.where(key_ok, sc, MASK_VALUE * LOG2E)
                top = jnp.max(sc, axis=0, keepdims=True)
                e = jnp.exp2(sc - top)
                e_s[pos] = e
                tops.append(top)
                sums.append(jnp.sum(e, axis=0, keepdims=True))
                pos += 1
        best = functools.reduce(jnp.maximum, tops)
        scales = [jnp.exp2(top - best) for top in tops]
        inv = 1.0 / functools.reduce(jnp.add, [f * l for f, l in zip(scales, sums)])
        probs = jnp.concatenate([(e_s[i] * (scales[i] * inv)).astype(BF16) for i in range(pos)], axis=0)
        mix = []
        for h in range(0, n_heads, 2):
            pair = dot(vt_s[h * head_dim:(h + 2) * head_dim, :], probs[:, h * tok_rows:(h + 2) * tok_rows])
            mix += [pair[:head_dim, :tok_rows], pair[head_dim:, tok_rows:]]
        attn = dot(wao_ts[b], (g * jnp.concatenate(mix, axis=0)).astype(BF16))
        acts = acts_s[...] + gate_s[k, b, 2] * attn
        normed = (gate_s[k, b, 3] * norm_cols(acts) + gate_s[k, b, 4]).astype(BF16)
        h = dot(wup_ts[b], normed)
        half = h.shape[0] // 2
        act = (silu(h[:half]) * h[half:]).astype(BF16)
        acts_s[...] = acts + gate_s[k, b, 5] * dot(wdown_ts[b], act)
        for copy in copies(r_s, k, *r_set) if rebuilt else copies(y_s, r, *y_set):
            copy.wait_send()

    turn(0)
    r_s[...] = jnp.zeros(r_s.shape, F32)
    for k in range(n_steps):
        if k > 0:
            r_s[k, me, :n_dim] = begin(k)
            for copy in copies(r_s, k, *r_set):
                copy.start()
            for off in range(1, n_peers):
                wait_from(u_s, k, *u_set, lax.rem(me + off, n_peers))
            u_all = jnp.concatenate([u_s[k, src] for src in range(n_peers)], axis=1)
            ast_all[...] = dot_tn(wstok_ref[...], u_all)
            mul_all[...] = sigmoid(dot_tn(wcond_ref[0, :, :c_token], u_all))
            add_all[...] = dot_tn(wcond_ref[0, :, c_token:2 * c_token], u_all)
        block(k, 0)
        for b in range(1, n_blocks):
            r = k * n_blocks + b
            y_s[r, me] = pack(k, b)
            for copy in copies(y_s, r, *y_set):
                copy.start()
            if k == 0:
                turn(b)
                if b == 1 and n_steps > 1:
                    gates(1, n_steps)
            block(k, b)
        if k == 0:
            for later in range(1, n_steps):
                for copy in copies(u_s, later, *u_set):
                    copy.wait_send()
        xn, t, var = noisy(k)
        update = dot(wout_ref[...], norm_cols(acts_s[...]).astype(BF16))
        denoised = (SIGMA_DATA * SIGMA_DATA / var) * xn + (t * SIGMA_DATA / jnp.sqrt(var)) * update
        xs_s[...] = xn + STEP_SCALE * (sig_ref[k + 1] - t) * (xn - denoised) / t
    out_ref[...] = xs_s[...]


def solution(mesh):
    part_axes = ("sample", "tok")
    n_peers = mesh.shape["tok"]

    def local_run(s_trunk, s_inputs, z_trunk, x_noise, step_noise, sigmas, relpos_table, w_pair_in, w_z_up, w_z_down, w_pair_bias, w_single, fourier_w, fourier_b, w_fourier, w_s_up, w_s_down, w_in, w_s_tok, w_cond, gate_bias, w_qkvg, w_attn_out, w_up, w_down, w_out):
        tok_rows, n_tok, c_pair = z_trunk.shape
        n_steps, _, n_dim = step_noise.shape
        n_blocks, _, n_heads = w_pair_bias.shape
        n_layers, _, width = w_z_up.shape
        c_token = w_qkvg.shape[1]
        clip = (relpos_table.shape[0] - 1) // 2
        tile = c_pair * SUB
        n_var = 2 * clip // SUB + LANES // SUB + 2
        n_rounds = n_steps * n_blocks
        swap = lambda a: jnp.swapaxes(a, -1, -2)
        ops = [
            sigmas, swap(z_trunk), swap(relpos_table), swap(w_pair_in), w_z_up, swap(w_z_down), swap(w_pair_bias),
            s_trunk, s_inputs, swap(x_noise), swap(step_noise), w_single, fourier_w[None, :], fourier_b[None, :], w_fourier, w_s_up, w_s_down,
            w_in, w_s_tok, w_cond, gate_bias, w_qkvg, w_attn_out, w_up, w_down, swap(w_out),
        ]
        specs = [pl.BlockSpec(memory_space=pltpu.SMEM), pl.BlockSpec(memory_space=pl.ANY)] + [pl.BlockSpec(memory_space=pltpu.VMEM)] * (len(ops) - 2)
        out = pl.pallas_call(
            functools.partial(kernel, "tok", n_peers),
            in_specs=specs,
            out_specs=pl.BlockSpec(memory_space=pltpu.VMEM),
            out_shape=jax.ShapeDtypeStruct((n_dim, tok_rows), F32),
            scratch_shapes=[
                pltpu.VMEM((tok_rows, c_pair, n_tok), BF16),
                pltpu.VMEM((n_blocks * n_heads, tok_rows, n_tok), F32),
                pltpu.VMEM((tile, 2 * tile), BF16),
                pltpu.VMEM((n_layers, width * SUB, tile), BF16),
                pltpu.VMEM((n_layers, tile, width // 2 * SUB), BF16),
                pltpu.VMEM((n_blocks * n_heads * SUB, tile), BF16),
                pltpu.VMEM((tile, tile), BF16),
                pltpu.VMEM((n_var, tile, LANES), F32),
                pltpu.VMEM((n_var, SUB, LANES), F32),
                pltpu.VMEM((2 * tile, CHUNK), BF16),
                pltpu.VMEM((n_layers + 1, tile, CHUNK), BF16),
                pltpu.VMEM((n_layers, tile, CHUNK), F32),
                pltpu.VMEM((n_layers, tile, CHUNK), F32),
                pltpu.VMEM((n_layers, width // 2 * SUB, CHUNK), BF16),
                pltpu.VMEM((n_blocks, n_tok, n_heads * tok_rows), F32),
                pltpu.VMEM((n_blocks, 4 * c_token, c_token), BF16),
                pltpu.VMEM((n_blocks, c_token, c_token), BF16),
                pltpu.VMEM((n_blocks, w_up.shape[2], c_token), BF16),
                pltpu.VMEM((n_blocks, c_token, w_down.shape[1]), BF16),
                pltpu.VMEM((c_token, SUB), F32),
                pltpu.VMEM((n_dim, c_token, tok_rows), F32),
                pltpu.VMEM((n_peers // 2, 2 * tok_rows, n_heads * tok_rows), F32),
                pltpu.VMEM((c_token, n_tok), BF16),
                pltpu.VMEM((c_token, tok_rows), F32),
                pltpu.VMEM((c_token, SUB), F32),
                pltpu.VMEM((n_steps, c_token, tok_rows), F32),
                pltpu.VMEM((n_steps, n_blocks, 6, c_token, tok_rows), F32),
                pltpu.VMEM((c_token, tok_rows), F32),
                pltpu.VMEM((n_dim, tok_rows), F32),
                pltpu.VMEM((n_rounds, n_peers, c_token, tok_rows), BF16),
                pltpu.VMEM((n_steps, c_token, tok_rows), BF16),
                pltpu.VMEM((n_steps, n_peers, c_token, tok_rows), BF16),
                pltpu.VMEM((n_steps, n_peers, SUB, tok_rows), F32),
                pltpu.VMEM((c_token, n_tok), F32),
                pltpu.VMEM((c_token, n_tok), F32),
                pltpu.VMEM((c_token, n_tok), F32),
                pltpu.SemaphoreType.DMA((2,)),
                pltpu.SemaphoreType.DMA((n_rounds, n_peers)),
                pltpu.SemaphoreType.DMA((n_rounds, n_peers)),
                pltpu.SemaphoreType.DMA((n_steps, n_peers)),
                pltpu.SemaphoreType.DMA((n_steps, n_peers)),
                pltpu.SemaphoreType.DMA((n_steps, n_peers)),
                pltpu.SemaphoreType.DMA((n_steps, n_peers)),
            ],
            compiler_params=pltpu.CompilerParams(collective_id=0, has_side_effects=True, vmem_limit_bytes=60 * 1024 * 1024),
            name="sampler",
        )(*ops)
        return swap(out)

    in_specs = (P("tok", None), P("tok", None), P("tok", None, None), P(part_axes, None), P(None, part_axes, None)) + (P(),) * 21
    return jax.shard_map(local_run, mesh=mesh, in_specs=in_specs, out_specs=P(part_axes, None), check_vma=False)
```

```python
import functools
import math
import jax
import jax.numpy as jnp
from jax import lax
from jax.experimental import pallas as pl
from jax.experimental.pallas import tpu as pltpu
from jax.sharding import PartitionSpec as P

SIGMA_DATA = 16.0
GAMMA = 0.8
NOISE_SCALE = 1.003
STEP_SCALE = 1.5
MASK_VALUE = -1e9
EPS = 1e-5
LOG2E = math.log2(math.e)
LANES = 128
SUB = 8
CHUNK = 256
UNROLL = 7
PACE = 4
SKEW = 2
GROUPS = ((0,), (2, 1, 3))
F32 = jnp.float32
BF16 = jnp.bfloat16


def dot(a, b):
    return jnp.dot(a, b, preferred_element_type=F32)


def dot_t(a, b):
    return lax.dot_general(a, b, (((1,), (1,)), ((), ())), preferred_element_type=F32)


def spread(n):
    rows = lax.broadcasted_iota(jnp.int32, (n * SUB, n), 0)
    cols = lax.broadcasted_iota(jnp.int32, (n * SUB, n), 1)
    return (rows // SUB == cols).astype(BF16)


def expand_tall(tall):
    full = dot_t(tall.astype(BF16), spread(tall.shape[1]))
    rows = lax.broadcasted_iota(jnp.int32, full.shape, 0) & (SUB - 1)
    cols = lax.broadcasted_iota(jnp.int32, full.shape, 1) & (SUB - 1)
    return jnp.where(rows == cols, full, 0.0)


def expand(weight):
    return expand_tall(dot(spread(weight.shape[0]), weight)).astype(BF16)


def norm_major(values):
    parts = values.reshape(values.shape[0] // SUB, SUB, values.shape[1])
    inv = 1.0 / parts.shape[0]
    centered = parts - jnp.sum(parts, axis=0, keepdims=True) * inv
    variance = jnp.sum(centered * centered, axis=0, keepdims=True) * inv
    return (centered * lax.rsqrt(variance + EPS)).reshape(values.shape).astype(BF16)


def dot_tn(a, b):
    return lax.dot_general(a, b, (((0,), (0,)), ((), ())), preferred_element_type=F32)


def norm_cols(values):
    inv = 1.0 / values.shape[0]
    centered = values - jnp.sum(values, axis=0, keepdims=True) * inv
    variance = jnp.sum(centered * centered, axis=0, keepdims=True) * inv
    return centered * lax.rsqrt(variance + EPS)


def norm_rows(values):
    inv = 1.0 / values.shape[-1]
    centered = values - jnp.sum(values, axis=-1, keepdims=True) * inv
    variance = jnp.sum(centered * centered, axis=-1, keepdims=True) * inv
    return centered * lax.rsqrt(variance + EPS)


def sigmoid(h):
    return 0.5 + 0.5 * jnp.tanh(0.5 * h)


def silu(h):
    half = 0.5 * h
    return half + half * jnp.tanh(half)


def weave(*parts):
    parts = list(parts)
    while parts:
        for part in list(parts):
            work, count = part
            if any(next(work, part) is part for _ in range(count)):
                parts.remove(part)


def kernel(
    axis, n_peers,
    sig_ref, z_hbm, rel_ref, pin_ref, zup_ref, zdown_ref, pb_ref,
    st_ref, si_ref, x_ref, noise_ref, wsingle_ref, fw_ref, fb_ref, wfour_ref, wsup_ref, wsdown_ref,
    win_ref, wstok_ref, wcond_ref, gbias_ref, wqkvg_ref, wao_ref, wup_ref, wdown_ref, wout_ref,
    out_ref,
    z_s, bias_s, pwin_s, pwup_s, pwdown_s, pwpb_s, perm_s, rel_s, relsum_s,
    zn_s, xn_ss, cond_ss, held_ss, act_ss,
    bias_ts, wqkvg_ts, wao_ts, wup_ts, wdown_ts, cols_s, win_s, e_s, vt_s,
    base_s, four_s, astok_s, gate_s, acts_s, xs_s, y_s, y_own, u_own, u_s, r_s, ast_all, mul_all, add_all,
    z_sem, y_send, y_recv, u_send, u_recv, r_send, r_recv,
):
    me = lax.axis_index(axis)
    tok_rows, c_pair, n_tok = z_hbm.shape
    n_layers = zup_ref.shape[0]
    n_bins = rel_ref.shape[1]
    clip = (n_bins - 1) // 2
    n_blocks, n_heads = pb_ref.shape[0], pb_ref.shape[1]
    c_token = st_ref.shape[1]
    head_dim = c_token // n_heads
    n_steps = noise_ref.shape[0]
    n_valid = n_tok - tok_rows // 4
    tile = c_pair * SUB
    n_var = rel_s.shape[0]
    low = (clip + SUB) // SUB

    first = SUB * pl.cdiv(2 + 2 * n_layers, n_tok // CHUNK)
    z_parts = [pl.ds(0, first), pl.ds(first, tok_rows - first)]
    z_copies = [pltpu.make_async_copy(z_hbm.at[part], z_s.at[part], z_sem.at[i]) for i, part in enumerate(z_parts)]
    for copy in z_copies:
        copy.start()
    barrier = pltpu.get_barrier_semaphore()
    for off in range(1, n_peers):
        pl.semaphore_signal(barrier, inc=1, device_id={axis: lax.rem(me + off, n_peers)}, device_id_type=pl.DeviceIdType.MESH)

    n_dim = x_ref.shape[0]

    def prepare():
        row = lax.broadcasted_iota(jnp.int32, (SUB, 1), 0)
        t_col = jnp.full((SUB, 1), sig_ref[0] * (1.0 + GAMMA), F32)
        for k in range(1, n_steps):
            t_col = jnp.where(row == k, sig_ref[k] * (1.0 + GAMMA), t_col)
        level = 0.25 * jnp.log(t_col / SIGMA_DATA)
        feat = jnp.cos(2.0 * math.pi * (level * fw_ref[...] + fb_ref[...]))
        yield
        four_s[...] = lax.dot_general(wfour_ref[...], norm_rows(feat).astype(BF16), (((0,), (1,)), ((), ())), preferred_element_type=F32)
        yield
        joined = norm_rows(jnp.concatenate([st_ref[...].astype(F32), si_ref[...].astype(F32)], axis=-1)).astype(BF16)
        base_s[...] = lax.dot_general(wsingle_ref[...], joined, (((0,), (1,)), ((), ())), preferred_element_type=F32)
        yield
        small = [gbias_ref[b] for b in range(n_blocks)] + [win_ref[...]]
        n_small = 2 * n_blocks + n_dim
        cols = jnp.transpose(jnp.concatenate(small + [jnp.zeros((-n_small % SUB, c_token), F32)], axis=0))
        cols_s[...] = cols
        for d in range(n_dim):
            win_s[d] = jnp.broadcast_to(cols[:, 2 * n_blocks + d:2 * n_blocks + d + 1], (c_token, tok_rows))
        yield
        yield from condition()

    def condition():
        single = jnp.concatenate([base_s[...] + four_s[:, k:k + 1] for k in range(n_steps)], axis=1)
        for layer in range(wsup_ref.shape[0]):
            h = dot_tn(wsup_ref[layer], norm_cols(single).astype(BF16))
            yield
            half = h.shape[0] // 2
            act = (silu(h[:half]) * h[half:]).astype(BF16)
            single = single + dot_tn(wsdown_ref[layer], act)
            yield
        u = norm_cols(single).astype(BF16)
        for k in range(n_steps):
            u_own[k] = u[:, k * tok_rows:(k + 1) * tok_rows]
        yield

    def gates(first, last):
        u = jnp.concatenate([u_own[k] for k in range(first, last)], axis=1)
        acts = dot_tn(wstok_ref[...], u)
        yield
        at = lambda v, k: v[:, (k - first) * tok_rows:(k - first + 1) * tok_rows]
        for k in range(first, last):
            astok_s[k] = at(acts, k)
        for b in range(n_blocks):
            cond = dot_tn(wcond_ref[b], u)
            yield
            part = lambda i: cond[i * c_token:(i + 1) * c_token]
            rows = [sigmoid(part(0)), part(1), sigmoid(part(2) + cols_s[:, 2 * b:2 * b + 1]), sigmoid(part(3)), part(4), sigmoid(part(5) + cols_s[:, 2 * b + 1:2 * b + 2])]
            for i, gate in enumerate(rows):
                for k in range(first, last):
                    gate_s[k, b, i] = at(gate, k)

    def copies(buf, i, send_sem, recv_sem):
        out = []
        for off in sorted(range(1, n_peers), key=lambda o: -min(o, n_peers - o)):
            peer = lax.rem(me + off, n_peers)
            out.append(pltpu.make_async_remote_copy(
                src_ref=buf.at[i, me], dst_ref=buf.at[i, me],
                send_sem=send_sem.at[i, off], recv_sem=recv_sem.at[i, me],
                device_id={axis: peer}, device_id_type=pl.DeviceIdType.MESH))
        return out

    def wait_from(buf, i, send_sem, recv_sem, src):
        pltpu.make_async_remote_copy(
            src_ref=buf.at[i, src], dst_ref=buf.at[i, src],
            send_sem=send_sem.at[i, 0], recv_sem=recv_sem.at[i, src],
            device_id={axis: src}, device_id_type=pl.DeviceIdType.MESH).wait_recv()

    y_set = (y_send, y_recv)
    u_set = (u_send, u_recv)
    r_set = (r_send, r_recv)

    def noisy(k):
        c = jnp.full((1, tok_rows), sig_ref[k], F32)
        t = c * (1.0 + GAMMA)
        xn = xs_s[...] + NOISE_SCALE * jnp.sqrt(t * t - c * c) * noise_ref[k]
        return xn, t, t * t + SIGMA_DATA * SIGMA_DATA

    def begin(k):
        xn, t, var = noisy(k)
        r = xn / jnp.sqrt(var)
        lin = r[0:1] * win_s[0]
        for d in range(1, n_dim):
            lin = lin + r[d:d + 1] * win_s[d]
        acts_s[...] = lin + astok_s[k]
        return r

    def pack(k, b):
        return (gate_s[k, b, 0] * norm_cols(acts_s[...]) + gate_s[k, b, 1]).astype(BF16)

    def tables():
        pin = pin_ref[...]
        pwin_s[:, :tile] = expand(pin[:, :c_pair])
        yield
        pwin_s[:, tile:] = expand(pin[:, c_pair:])
        yield
        for layer in range(n_layers):
            up = zup_ref[layer]
            width = up.shape[1]
            full = expand_tall(dot_t(spread(width), up))
            gate_rows = lax.broadcasted_iota(jnp.int32, full.shape, 0) < (width // 2) * SUB
            pwup_s[layer] = jnp.where(gate_rows, 0.5 * full, full).astype(BF16)
            yield
            pwdown_s[layer] = expand(zdown_ref[layer])
            yield
        for b in range(n_blocks):
            pwpb_s[b * n_heads * SUB:(b + 1) * n_heads * SUB, :] = expand(pb_ref[b])
            yield
        rows_i = lax.broadcasted_iota(jnp.int32, (tile, tile), 0)
        cols_i = lax.broadcasted_iota(jnp.int32, (tile, tile), 1)
        perm_s[...] = ((rows_i & (SUB - 1)) * c_pair + rows_i // SUB == cols_i).astype(BF16)
        yield
        tall = dot(spread(c_pair), rel_ref[...]).astype(BF16)
        bin_i = lax.broadcasted_iota(jnp.int32, (n_bins, LANES), 0)
        diag_i = lax.broadcasted_iota(jnp.int32, (n_bins, LANES), 1)
        row_s = lax.broadcasted_iota(jnp.int32, (tile, LANES), 0) & (SUB - 1)
        tab = jnp.zeros((tile, LANES), F32)
        for s in range(SUB):
            pick = (bin_i == jnp.clip(diag_i - (SUB - 1) + s, 0, n_bins - 1)).astype(BF16)
            tab = jnp.where(row_s == s, dot(tall, pick), tab)
            yield
        tab = tab.astype(BF16)

        per = 2
        k_i = lax.broadcasted_iota(jnp.int32, (LANES, LANES), 0)
        j_i = lax.broadcasted_iota(jnp.int32, (LANES, LANES), 1)

        for i in range(0, n_var, per):
            picks = []
            for v in range(i, i + per):
                want = jnp.clip(SUB * (v - low) - j_i + clip + SUB - 1, 0, n_bins + SUB - 2)
                picks.append((k_i == want).astype(BF16))
            planes = dot(tab, jnp.concatenate(picks, axis=1))
            yield
            for v in range(i, i + per):
                plane = planes[:, (v - i) * LANES:(v - i + 1) * LANES]
                rel_s[v] = plane
                relsum_s[v] = jnp.sum(plane.reshape(c_pair, SUB, LANES), axis=0)

    n_chunks = n_tok // CHUNK
    total = (tok_rows // SUB) * n_chunks
    depth = 2 + 2 * n_layers

    def trip(it):
        known = isinstance(it, int)

        def active(lag):
            return not known or 0 <= it - lag < total

        def place(lag):
            idx = it - lag
            r0, c0 = (idx // n_chunks) * SUB, (idx % n_chunks) * CHUNK
            return (r0, c0) if known else (pl.multiple_of(r0, SUB), pl.multiple_of(c0, CHUNK))

        def out_store(bias):
            r0, c0 = place(depth)
            bias = bias.astype(BF16).astype(F32) * LOG2E
            bias_s[:, pl.ds(r0, SUB), pl.ds(c0, CHUNK)] = bias.reshape(n_blocks * n_heads, SUB, CHUNK)

        def down_store(layer, cond):
            xn_ss[layer + 1] = norm_major(cond)
            if layer + 1 < n_layers:
                cond_ss[layer + 1] = cond

        def up_store(layer, h):
            half = h.shape[0] // 2
            gate = h[:half]
            act_ss[layer] = ((gate + gate * jnp.tanh(gate)) * h[half:]).astype(BF16)
            held_ss[layer] = cond_ss[layer]

        def in_store(cond):
            cond_ss[0] = cond
            xn_ss[0] = norm_major(cond)

        def turn_rows():
            r0, c0 = place(0)
            zb = z_s[pl.ds(r0, SUB), :, pl.ds(c0, CHUNK)].reshape(tile, CHUNK)
            return dot(perm_s[...], zb).reshape(c_pair, SUB, CHUNK)

        def pair_store(z):
            r0, c0 = place(0)
            rels, sums = [], []
            for part in range(CHUNK // LANES):
                delta = me * tok_rows + r0 - c0 - part * LANES
                v = jnp.clip(delta // SUB + low, 0, n_var - 1)
                rels.append(rel_s[v])
                sums.append(relsum_s[v])
            rel = jnp.concatenate(rels, axis=1).reshape(c_pair, SUB, CHUNK)
            inv = 1.0 / (2 * c_pair)
            mean = (jnp.sum(z, axis=0) + jnp.concatenate(sums, axis=1)) * inv
            zc = z - mean
            rc = rel - mean
            var = (jnp.sum(zc * zc, axis=0) + jnp.sum(rc * rc, axis=0)) * inv
            rs = lax.rsqrt(var + EPS)
            zn_s[:tile] = (zc * rs).reshape(tile, CHUNK).astype(BF16)
            zn_s[tile:] = (rc * rs).reshape(tile, CHUNK).astype(BF16)

        stages = []
        if active(depth):
            stages.append((lambda: dot(pwpb_s[...], xn_ss[n_layers]), out_store))
        for layer in reversed(range(n_layers)):
            if active(3 + 2 * layer):
                stages.append((lambda layer=layer: held_ss[layer] + dot(pwdown_s[layer], act_ss[layer]), functools.partial(down_store, layer)))
            if active(2 + 2 * layer):
                stages.append((lambda layer=layer: dot(pwup_s[layer], xn_ss[layer]), functools.partial(up_store, layer)))
        if active(1):
            stages.append((lambda: dot(pwin_s[...], zn_s[...]), in_store))
        if active(0):
            stages.append((turn_rows, pair_store))
        return stages

    def run(its):
        waiting = []
        for it in its:
            stages = trip(it)
            for first_half, second_half in stages:
                waiting.append(functools.partial(second_half, first_half()))
                if len(waiting) > SKEW:
                    waiting.pop(0)()
            while waiting and len(stages) < SKEW + 2:
                waiting.pop(0)()
            yield
        for rest in waiting:
            rest()

    loops = (total - depth) // UNROLL

    def trips(i, carry):
        weave((run([depth + i * UNROLL + j for j in range(UNROLL)]), 1))
        return carry

    def turned():
        for b in range(n_blocks):
            for src, dst in ((wqkvg_ref, wqkvg_ts), (wao_ref, wao_ts), (wup_ref, wup_ts), (wdown_ref, wdown_ts)):
                dst[b] = jnp.transpose(src[b])
                yield

    weave((prepare(), 1), (tables(), PACE), (turned(), 1))
    z_copies[0].wait()

    def start():
        yield from gates(0, 1)
        xs_s[...] = sig_ref[0] * x_ref[...]
        begin(0)
        yield
        y_own[...] = pack(0, 0)

    weave((start(), 1), (run(range(depth)), 1))
    y_s[0, me] = y_own[...]
    for k in range(1, n_steps):
        u_s[k, me] = u_own[k]
    pl.semaphore_wait(barrier, n_peers - 1)
    for copy in copies(y_s, 0, *y_set):
        copy.start()
    for k in range(1, n_steps):
        for copy in copies(u_s, k, *u_set):
            copy.start()
    z_copies[1].wait()
    lax.fori_loop(0, loops, trips, 0)
    weave((run(range(depth + loops * UNROLL, total + depth)), 1))

    def turn(b):
        for h in range(n_heads):
            for key0 in range(0, n_tok, LANES):
                bias_ts[b, key0:key0 + LANES, h * tok_rows:(h + 1) * tok_rows] = jnp.transpose(bias_s[b * n_heads + h, :, key0:key0 + LANES])

    head = lax.broadcasted_iota(jnp.int32, (c_token, 1), 0) // head_dim
    scale = head_dim ** -0.5 * LOG2E
    cores = 2
    n_chips = n_peers // cores
    chip_keys = cores * tok_rows
    my_chip = me // cores

    def others(d, chip):
        return [me + 1 - 2 * lax.rem(me, cores)] if d == 0 else [chip * cores + c for c in range(cores)]

    def block(k, b):
        r = k * n_blocks + b
        rebuilt = k > 0 and b == 0
        y = pack(k, b) if rebuilt else y_s[r, me]
        q = dot(wqkvg_ts[b, :c_token, :], y)
        g = sigmoid(dot(wqkvg_ts[b, 3 * c_token:, :], y))
        q_heads = jnp.concatenate([jnp.where(head == h, q, 0.0).astype(BF16) for h in range(n_heads)], axis=1)
        tops, sums = [], []
        pos = 0
        for group in GROUPS if r > 0 else (sum(GROUPS, ()),):
            chips = [lax.rem(my_chip + d, n_chips) for d in group]
            for d, chip in zip(group, chips):
                for src in others(d, chip):
                    if rebuilt:
                        wait_from(r_s, k, *r_set, src)
                    else:
                        wait_from(y_s, r, *y_set, src)
            if rebuilt:
                parts = []
                for chip in chips:
                    keys = pl.ds(pl.multiple_of(chip * chip_keys, chip_keys), chip_keys)
                    pos_r = jnp.concatenate([r_s[k, chip * cores + c] for c in range(cores)], axis=1)
                    lin = pos_r[0:1] * jnp.concatenate([win_s[0]] * cores, axis=1)
                    for d in range(1, n_dim):
                        lin = lin + pos_r[d:d + 1] * jnp.concatenate([win_s[d]] * cores, axis=1)
                    parts.append((mul_all[:, keys] * norm_cols(lin + ast_all[:, keys]) + add_all[:, keys]).astype(BF16))
                y_group = jnp.concatenate(parts, axis=1)
            else:
                y_group = jnp.concatenate([y_s[r, chip * cores + c] for chip in chips for c in range(cores)], axis=1)
            kv = dot(wqkvg_ts[b, c_token:3 * c_token, :], y_group).astype(BF16)
            vt_s[:, pos * chip_keys:(pos + len(group)) * chip_keys] = kv[c_token:]
            scores = dot_tn(kv[:c_token], q_heads)
            for i, chip in enumerate(chips):
                key0 = pl.multiple_of(chip * chip_keys, chip_keys)
                sc = scores[i * chip_keys:(i + 1) * chip_keys] * scale + bias_ts[b, pl.ds(key0, chip_keys), :]
                key_ok = lax.broadcasted_iota(jnp.int32, (chip_keys, 1), 0) + key0 < n_valid
                sc = jnp.where(key_ok, sc, MASK_VALUE * LOG2E)
                top = jnp.max(sc, axis=0, keepdims=True)
                e = jnp.exp2(sc - top)
                e_s[pos] = e
                tops.append(top)
                sums.append(jnp.sum(e, axis=0, keepdims=True))
                pos += 1
        best = functools.reduce(jnp.maximum, tops)
        scales = [jnp.exp2(top - best) for top in tops]
        inv = 1.0 / functools.reduce(jnp.add, [f * l for f, l in zip(scales, sums)])
        probs = jnp.concatenate([(e_s[i] * (scales[i] * inv)).astype(BF16) for i in range(pos)], axis=0)
        mix = []
        for h in range(0, n_heads, 2):
            pair = dot(vt_s[h * head_dim:(h + 2) * head_dim, :], probs[:, h * tok_rows:(h + 2) * tok_rows])
            mix += [pair[:head_dim, :tok_rows], pair[head_dim:, tok_rows:]]
        attn = dot(wao_ts[b], (g * jnp.concatenate(mix, axis=0)).astype(BF16))
        acts = acts_s[...] + gate_s[k, b, 2] * attn
        normed = (gate_s[k, b, 3] * norm_cols(acts) + gate_s[k, b, 4]).astype(BF16)
        h = dot(wup_ts[b], normed)
        half = h.shape[0] // 2
        act = (silu(h[:half]) * h[half:]).astype(BF16)
        acts_s[...] = acts + gate_s[k, b, 5] * dot(wdown_ts[b], act)
        for copy in copies(r_s, k, *r_set) if rebuilt else copies(y_s, r, *y_set):
            copy.wait_send()

    turn(0)
    r_s[...] = jnp.zeros(r_s.shape, F32)
    for k in range(n_steps):
        if k > 0:
            r_s[k, me, :n_dim] = begin(k)
            for copy in copies(r_s, k, *r_set):
                copy.start()
            for off in range(1, n_peers):
                wait_from(u_s, k, *u_set, lax.rem(me + off, n_peers))
            u_all = jnp.concatenate([u_s[k, src] for src in range(n_peers)], axis=1)
            ast_all[...] = dot_tn(wstok_ref[...], u_all)
            mul_all[...] = sigmoid(dot_tn(wcond_ref[0, :, :c_token], u_all))
            add_all[...] = dot_tn(wcond_ref[0, :, c_token:2 * c_token], u_all)
        block(k, 0)
        for b in range(1, n_blocks):
            r = k * n_blocks + b
            y_s[r, me] = pack(k, b)
            for copy in copies(y_s, r, *y_set):
                copy.start()
            if k == 0:
                turn(b)
                if b == 1 and n_steps > 1:
                    weave((gates(1, n_steps), 1))
            block(k, b)
        if k == 0:
            for later in range(1, n_steps):
                for copy in copies(u_s, later, *u_set):
                    copy.wait_send()
        xn, t, var = noisy(k)
        update = dot(wout_ref[...], norm_cols(acts_s[...]).astype(BF16))
        denoised = (SIGMA_DATA * SIGMA_DATA / var) * xn + (t * SIGMA_DATA / jnp.sqrt(var)) * update
        xs_s[...] = xn + STEP_SCALE * (sig_ref[k + 1] - t) * (xn - denoised) / t
    out_ref[...] = xs_s[...]


def solution(mesh):
    part_axes = ("sample", "tok")
    n_peers = mesh.shape["tok"]

    def local_run(s_trunk, s_inputs, z_trunk, x_noise, step_noise, sigmas, relpos_table, w_pair_in, w_z_up, w_z_down, w_pair_bias, w_single, fourier_w, fourier_b, w_fourier, w_s_up, w_s_down, w_in, w_s_tok, w_cond, gate_bias, w_qkvg, w_attn_out, w_up, w_down, w_out):
        tok_rows, n_tok, c_pair = z_trunk.shape
        n_steps, _, n_dim = step_noise.shape
        n_blocks, _, n_heads = w_pair_bias.shape
        n_layers, _, width = w_z_up.shape
        c_token = w_qkvg.shape[1]
        clip = (relpos_table.shape[0] - 1) // 2
        tile = c_pair * SUB
        n_var = 2 * clip // SUB + LANES // SUB + 2
        n_rounds = n_steps * n_blocks
        swap = lambda a: jnp.swapaxes(a, -1, -2)
        ops = [
            sigmas, swap(z_trunk), swap(relpos_table), swap(w_pair_in), w_z_up, swap(w_z_down), swap(w_pair_bias),
            s_trunk, s_inputs, swap(x_noise), swap(step_noise), w_single, fourier_w[None, :], fourier_b[None, :], w_fourier, w_s_up, w_s_down,
            w_in, w_s_tok, w_cond, gate_bias, w_qkvg, w_attn_out, w_up, w_down, swap(w_out),
        ]
        specs = [pl.BlockSpec(memory_space=pltpu.SMEM), pl.BlockSpec(memory_space=pl.ANY)] + [pl.BlockSpec(memory_space=pltpu.VMEM)] * (len(ops) - 2)
        out = pl.pallas_call(
            functools.partial(kernel, "tok", n_peers),
            in_specs=specs,
            out_specs=pl.BlockSpec(memory_space=pltpu.VMEM),
            out_shape=jax.ShapeDtypeStruct((n_dim, tok_rows), F32),
            scratch_shapes=[
                pltpu.VMEM((tok_rows, c_pair, n_tok), BF16),
                pltpu.VMEM((n_blocks * n_heads, tok_rows, n_tok), F32),
                pltpu.VMEM((tile, 2 * tile), BF16),
                pltpu.VMEM((n_layers, width * SUB, tile), BF16),
                pltpu.VMEM((n_layers, tile, width // 2 * SUB), BF16),
                pltpu.VMEM((n_blocks * n_heads * SUB, tile), BF16),
                pltpu.VMEM((tile, tile), BF16),
                pltpu.VMEM((n_var, tile, LANES), F32),
                pltpu.VMEM((n_var, SUB, LANES), F32),
                pltpu.VMEM((2 * tile, CHUNK), BF16),
                pltpu.VMEM((n_layers + 1, tile, CHUNK), BF16),
                pltpu.VMEM((n_layers, tile, CHUNK), F32),
                pltpu.VMEM((n_layers, tile, CHUNK), F32),
                pltpu.VMEM((n_layers, width // 2 * SUB, CHUNK), BF16),
                pltpu.VMEM((n_blocks, n_tok, n_heads * tok_rows), F32),
                pltpu.VMEM((n_blocks, 4 * c_token, c_token), BF16),
                pltpu.VMEM((n_blocks, c_token, c_token), BF16),
                pltpu.VMEM((n_blocks, w_up.shape[2], c_token), BF16),
                pltpu.VMEM((n_blocks, c_token, w_down.shape[1]), BF16),
                pltpu.VMEM((c_token, SUB), F32),
                pltpu.VMEM((n_dim, c_token, tok_rows), F32),
                pltpu.VMEM((n_peers // 2, 2 * tok_rows, n_heads * tok_rows), F32),
                pltpu.VMEM((c_token, n_tok), BF16),
                pltpu.VMEM((c_token, tok_rows), F32),
                pltpu.VMEM((c_token, SUB), F32),
                pltpu.VMEM((n_steps, c_token, tok_rows), F32),
                pltpu.VMEM((n_steps, n_blocks, 6, c_token, tok_rows), F32),
                pltpu.VMEM((c_token, tok_rows), F32),
                pltpu.VMEM((n_dim, tok_rows), F32),
                pltpu.VMEM((n_rounds, n_peers, c_token, tok_rows), BF16),
                pltpu.VMEM((c_token, tok_rows), BF16),
                pltpu.VMEM((n_steps, c_token, tok_rows), BF16),
                pltpu.VMEM((n_steps, n_peers, c_token, tok_rows), BF16),
                pltpu.VMEM((n_steps, n_peers, SUB, tok_rows), F32),
                pltpu.VMEM((c_token, n_tok), F32),
                pltpu.VMEM((c_token, n_tok), F32),
                pltpu.VMEM((c_token, n_tok), F32),
                pltpu.SemaphoreType.DMA((2,)),
                pltpu.SemaphoreType.DMA((n_rounds, n_peers)),
                pltpu.SemaphoreType.DMA((n_rounds, n_peers)),
                pltpu.SemaphoreType.DMA((n_steps, n_peers)),
                pltpu.SemaphoreType.DMA((n_steps, n_peers)),
                pltpu.SemaphoreType.DMA((n_steps, n_peers)),
                pltpu.SemaphoreType.DMA((n_steps, n_peers)),
            ],
            compiler_params=pltpu.CompilerParams(collective_id=0, has_side_effects=True, vmem_limit_bytes=60 * 1024 * 1024),
            name="sampler",
        )(*ops)
        return swap(out)

    in_specs = (P("tok", None), P("tok", None), P("tok", None, None), P(part_axes, None), P(None, part_axes, None)) + (P(),) * 21
    return jax.shard_map(local_run, mesh=mesh, in_specs=in_specs, out_specs=P(part_axes, None), check_vma=False)
```

```python
import functools
import math
import jax
import jax.numpy as jnp
from jax import lax
from jax.experimental import pallas as pl
from jax.experimental.pallas import tpu as pltpu
from jax.sharding import PartitionSpec as P

SIGMA_DATA = 16.0
GAMMA = 0.8
NOISE_SCALE = 1.003
STEP_SCALE = 1.5
MASK_VALUE = -1e9
EPS = 1e-5
LOG2E = math.log2(math.e)
LANES = 128
SUB = 8
CHUNK = 512
UNROLL = 4
PACE = 4
SKEW = 2
GROUPS = ((0,), (2, 1, 3))
F32 = jnp.float32
BF16 = jnp.bfloat16


def dot(a, b):
    return jnp.dot(a, b, preferred_element_type=F32)


def dot_t(a, b):
    return lax.dot_general(a, b, (((1,), (1,)), ((), ())), preferred_element_type=F32)


def spread(n):
    rows = lax.broadcasted_iota(jnp.int32, (n * SUB, n), 0)
    cols = lax.broadcasted_iota(jnp.int32, (n * SUB, n), 1)
    return (rows // SUB == cols).astype(BF16)


def expand_tall(tall):
    full = dot_t(tall.astype(BF16), spread(tall.shape[1]))
    rows = lax.broadcasted_iota(jnp.int32, full.shape, 0) & (SUB - 1)
    cols = lax.broadcasted_iota(jnp.int32, full.shape, 1) & (SUB - 1)
    return jnp.where(rows == cols, full, 0.0)


def expand(weight):
    return expand_tall(dot(spread(weight.shape[0]), weight)).astype(BF16)


def norm_major(values):
    parts = values.reshape(values.shape[0] // SUB, SUB, values.shape[1])
    inv = 1.0 / parts.shape[0]
    centered = parts - jnp.sum(parts, axis=0, keepdims=True) * inv
    variance = jnp.sum(centered * centered, axis=0, keepdims=True) * inv
    return (centered * lax.rsqrt(variance + EPS)).reshape(values.shape).astype(BF16)


def dot_tn(a, b):
    return lax.dot_general(a, b, (((0,), (0,)), ((), ())), preferred_element_type=F32)


def norm_cols(values):
    inv = 1.0 / values.shape[0]
    centered = values - jnp.sum(values, axis=0, keepdims=True) * inv
    variance = jnp.sum(centered * centered, axis=0, keepdims=True) * inv
    return centered * lax.rsqrt(variance + EPS)


def norm_rows(values):
    inv = 1.0 / values.shape[-1]
    centered = values - jnp.sum(values, axis=-1, keepdims=True) * inv
    variance = jnp.sum(centered * centered, axis=-1, keepdims=True) * inv
    return centered * lax.rsqrt(variance + EPS)


def sigmoid(h):
    return 0.5 + 0.5 * jnp.tanh(0.5 * h)


def silu(h):
    half = 0.5 * h
    return half + half * jnp.tanh(half)


def weave(*parts):
    parts = list(parts)
    while parts:
        for part in list(parts):
            work, count = part
            if any(next(work, part) is part for _ in range(count)):
                parts.remove(part)


def kernel(
    axis, n_peers,
    sig_ref, z_hbm, rel_ref, pin_ref, zup_ref, zdown_ref, pb_ref,
    st_ref, si_ref, x_ref, noise_ref, wsingle_ref, fw_ref, fb_ref, wfour_ref, wsup_ref, wsdown_ref,
    win_ref, wstok_ref, wcond_ref, gbias_ref, wqkvg_ref, wao_ref, wup_ref, wdown_ref, wout_ref,
    out_ref,
    z_s, bias_s, pwin_s, pwup_s, pwdown_s, pwpb_s, perm_s, rel_s, relsum_s,
    zn_s, xn_ss, cond_ss, held_ss, act_ss,
    bias_ts, wqkvg_ts, wao_ts, wup_ts, wdown_ts, cols_s, win_s, e_s, vt_s,
    base_s, four_s, astok_s, gate_s, acts_s, xs_s, y_s, y_own, u_own, u_s, r_s, ast_all, mul_all, add_all,
    z_sem, y_send, y_recv, u_send, u_recv, r_send, r_recv,
):
    me = lax.axis_index(axis)
    tok_rows, c_pair, n_tok = z_hbm.shape
    n_layers = zup_ref.shape[0]
    n_bins = rel_ref.shape[1]
    clip = (n_bins - 1) // 2
    n_blocks, n_heads = pb_ref.shape[0], pb_ref.shape[1]
    c_token = st_ref.shape[1]
    head_dim = c_token // n_heads
    n_steps = noise_ref.shape[0]
    n_valid = n_tok - tok_rows // 4
    tile = c_pair * SUB
    n_var = rel_s.shape[0]
    low = (clip + SUB) // SUB

    first = SUB * pl.cdiv(2 + 2 * n_layers, n_tok // CHUNK)
    z_parts = [pl.ds(0, first), pl.ds(first, tok_rows - first)]
    z_copies = [pltpu.make_async_copy(z_hbm.at[part], z_s.at[part], z_sem.at[i]) for i, part in enumerate(z_parts)]
    for copy in z_copies:
        copy.start()
    barrier = pltpu.get_barrier_semaphore()
    for off in range(1, n_peers):
        pl.semaphore_signal(barrier, inc=1, device_id={axis: lax.rem(me + off, n_peers)}, device_id_type=pl.DeviceIdType.MESH)

    n_dim = x_ref.shape[0]

    def prepare():
        row = lax.broadcasted_iota(jnp.int32, (SUB, 1), 0)
        t_col = jnp.full((SUB, 1), sig_ref[0] * (1.0 + GAMMA), F32)
        for k in range(1, n_steps):
            t_col = jnp.where(row == k, sig_ref[k] * (1.0 + GAMMA), t_col)
        level = 0.25 * jnp.log(t_col / SIGMA_DATA)
        feat = jnp.cos(2.0 * math.pi * (level * fw_ref[...] + fb_ref[...]))
        yield
        four_s[...] = lax.dot_general(wfour_ref[...], norm_rows(feat).astype(BF16), (((0,), (1,)), ((), ())), preferred_element_type=F32)
        yield
        joined = norm_rows(jnp.concatenate([st_ref[...].astype(F32), si_ref[...].astype(F32)], axis=-1)).astype(BF16)
        base_s[...] = lax.dot_general(wsingle_ref[...], joined, (((0,), (1,)), ((), ())), preferred_element_type=F32)
        yield
        small = [gbias_ref[b] for b in range(n_blocks)] + [win_ref[...]]
        n_small = 2 * n_blocks + n_dim
        cols = jnp.transpose(jnp.concatenate(small + [jnp.zeros((-n_small % SUB, c_token), F32)], axis=0))
        cols_s[...] = cols
        for d in range(n_dim):
            win_s[d] = jnp.broadcast_to(cols[:, 2 * n_blocks + d:2 * n_blocks + d + 1], (c_token, tok_rows))
        yield
        yield from condition()

    def condition():
        single = jnp.concatenate([base_s[...] + four_s[:, k:k + 1] for k in range(n_steps)], axis=1)
        for layer in range(wsup_ref.shape[0]):
            h = dot_tn(wsup_ref[layer], norm_cols(single).astype(BF16))
            yield
            half = h.shape[0] // 2
            act = (silu(h[:half]) * h[half:]).astype(BF16)
            single = single + dot_tn(wsdown_ref[layer], act)
            yield
        u = norm_cols(single).astype(BF16)
        for k in range(n_steps):
            u_own[k] = u[:, k * tok_rows:(k + 1) * tok_rows]
        yield

    def gates(first, last):
        u = jnp.concatenate([u_own[k] for k in range(first, last)], axis=1)
        acts = dot_tn(wstok_ref[...], u)
        yield
        at = lambda v, k: v[:, (k - first) * tok_rows:(k - first + 1) * tok_rows]
        for k in range(first, last):
            astok_s[k] = at(acts, k)
        for b in range(n_blocks):
            cond = dot_tn(wcond_ref[b], u)
            yield
            part = lambda i: cond[i * c_token:(i + 1) * c_token]
            rows = [sigmoid(part(0)), part(1), sigmoid(part(2) + cols_s[:, 2 * b:2 * b + 1]), sigmoid(part(3)), part(4), sigmoid(part(5) + cols_s[:, 2 * b + 1:2 * b + 2])]
            for i, gate in enumerate(rows):
                for k in range(first, last):
                    gate_s[k, b, i] = at(gate, k)

    def copies(buf, i, send_sem, recv_sem):
        out = []
        for off in sorted(range(1, n_peers), key=lambda o: -min(o, n_peers - o)):
            peer = lax.rem(me + off, n_peers)
            out.append(pltpu.make_async_remote_copy(
                src_ref=buf.at[i, me], dst_ref=buf.at[i, me],
                send_sem=send_sem.at[i, off], recv_sem=recv_sem.at[i, me],
                device_id={axis: peer}, device_id_type=pl.DeviceIdType.MESH))
        return out

    def wait_from(buf, i, send_sem, recv_sem, src):
        pltpu.make_async_remote_copy(
            src_ref=buf.at[i, src], dst_ref=buf.at[i, src],
            send_sem=send_sem.at[i, 0], recv_sem=recv_sem.at[i, src],
            device_id={axis: src}, device_id_type=pl.DeviceIdType.MESH).wait_recv()

    y_set = (y_send, y_recv)
    u_set = (u_send, u_recv)
    r_set = (r_send, r_recv)

    def noisy(k):
        c = jnp.full((1, tok_rows), sig_ref[k], F32)
        t = c * (1.0 + GAMMA)
        xn = xs_s[...] + NOISE_SCALE * jnp.sqrt(t * t - c * c) * noise_ref[k]
        return xn, t, t * t + SIGMA_DATA * SIGMA_DATA

    def begin(k):
        xn, t, var = noisy(k)
        r = xn / jnp.sqrt(var)
        lin = r[0:1] * win_s[0]
        for d in range(1, n_dim):
            lin = lin + r[d:d + 1] * win_s[d]
        acts_s[...] = lin + astok_s[k]
        return r

    def pack(k, b):
        return (gate_s[k, b, 0] * norm_cols(acts_s[...]) + gate_s[k, b, 1]).astype(BF16)

    def tables():
        pin = pin_ref[...]
        pwin_s[:, :tile] = expand(pin[:, :c_pair])
        yield
        pwin_s[:, tile:] = expand(pin[:, c_pair:])
        yield
        for layer in range(n_layers):
            up = zup_ref[layer]
            width = up.shape[1]
            full = expand_tall(dot_t(spread(width), up))
            gate_rows = lax.broadcasted_iota(jnp.int32, full.shape, 0) < (width // 2) * SUB
            pwup_s[layer] = jnp.where(gate_rows, 0.5 * full, full).astype(BF16)
            yield
            pwdown_s[layer] = expand(zdown_ref[layer])
            yield
        for b in range(n_blocks):
            pwpb_s[b * n_heads * SUB:(b + 1) * n_heads * SUB, :] = expand(pb_ref[b])
            yield
        rows_i = lax.broadcasted_iota(jnp.int32, (tile, tile), 0)
        cols_i = lax.broadcasted_iota(jnp.int32, (tile, tile), 1)
        perm_s[...] = ((rows_i & (SUB - 1)) * c_pair + rows_i // SUB == cols_i).astype(BF16)
        yield
        tall = dot(spread(c_pair), rel_ref[...]).astype(BF16)
        bin_i = lax.broadcasted_iota(jnp.int32, (n_bins, LANES), 0)
        diag_i = lax.broadcasted_iota(jnp.int32, (n_bins, LANES), 1)
        row_s = lax.broadcasted_iota(jnp.int32, (tile, LANES), 0) & (SUB - 1)
        tab = jnp.zeros((tile, LANES), F32)
        for s in range(SUB):
            pick = (bin_i == jnp.clip(diag_i - (SUB - 1) + s, 0, n_bins - 1)).astype(BF16)
            tab = jnp.where(row_s == s, dot(tall, pick), tab)
            yield
        tab = tab.astype(BF16)

        per = 2
        k_i = lax.broadcasted_iota(jnp.int32, (LANES, LANES), 0)
        j_i = lax.broadcasted_iota(jnp.int32, (LANES, LANES), 1)

        for i in range(0, n_var, per):
            picks = []
            for v in range(i, i + per):
                want = jnp.clip(SUB * (v - low) - j_i + clip + SUB - 1, 0, n_bins + SUB - 2)
                picks.append((k_i == want).astype(BF16))
            planes = dot(tab, jnp.concatenate(picks, axis=1))
            yield
            for v in range(i, i + per):
                plane = planes[:, (v - i) * LANES:(v - i + 1) * LANES]
                rel_s[v] = plane
                relsum_s[v] = jnp.sum(plane.reshape(c_pair, SUB, LANES), axis=0)

    n_chunks = n_tok // CHUNK
    total = (tok_rows // SUB) * n_chunks
    depth = 2 + 2 * n_layers

    def trip(it):
        known = isinstance(it, int)

        def active(lag):
            return not known or 0 <= it - lag < total

        def place(lag):
            idx = it - lag
            r0, c0 = (idx // n_chunks) * SUB, (idx % n_chunks) * CHUNK
            return (r0, c0) if known else (pl.multiple_of(r0, SUB), pl.multiple_of(c0, CHUNK))

        def out_store(bias):
            r0, c0 = place(depth)
            bias = bias.astype(BF16).astype(F32) * LOG2E
            bias_s[:, pl.ds(r0, SUB), pl.ds(c0, CHUNK)] = bias.reshape(n_blocks * n_heads, SUB, CHUNK)

        def down_store(layer, cond):
            xn_ss[layer + 1] = norm_major(cond)
            if layer + 1 < n_layers:
                cond_ss[layer + 1] = cond

        def up_store(layer, h):
            half = h.shape[0] // 2
            gate = h[:half]
            act_ss[layer] = ((gate + gate * jnp.tanh(gate)) * h[half:]).astype(BF16)
            held_ss[layer] = cond_ss[layer]

        def in_store(cond):
            cond_ss[0] = cond
            xn_ss[0] = norm_major(cond)

        def turn_rows():
            r0, c0 = place(0)
            zb = z_s[pl.ds(r0, SUB), :, pl.ds(c0, CHUNK)].reshape(tile, CHUNK)
            return dot(perm_s[...], zb).reshape(c_pair, SUB, CHUNK)

        def pair_store(z):
            r0, c0 = place(0)
            rels, sums = [], []
            for part in range(CHUNK // LANES):
                delta = me * tok_rows + r0 - c0 - part * LANES
                v = jnp.clip(delta // SUB + low, 0, n_var - 1)
                rels.append(rel_s[v])
                sums.append(relsum_s[v])
            rel = jnp.concatenate(rels, axis=1).reshape(c_pair, SUB, CHUNK)
            inv = 1.0 / (2 * c_pair)
            mean = (jnp.sum(z, axis=0) + jnp.concatenate(sums, axis=1)) * inv
            zc = z - mean
            rc = rel - mean
            var = (jnp.sum(zc * zc, axis=0) + jnp.sum(rc * rc, axis=0)) * inv
            rs = lax.rsqrt(var + EPS)
            zn_s[:tile] = (zc * rs).reshape(tile, CHUNK).astype(BF16)
            zn_s[tile:] = (rc * rs).reshape(tile, CHUNK).astype(BF16)

        stages = []
        if active(depth):
            stages.append((lambda: dot(pwpb_s[...], xn_ss[n_layers]), out_store))
        for layer in reversed(range(n_layers)):
            if active(3 + 2 * layer):
                stages.append((lambda layer=layer: held_ss[layer] + dot(pwdown_s[layer], act_ss[layer]), functools.partial(down_store, layer)))
            if active(2 + 2 * layer):
                stages.append((lambda layer=layer: dot(pwup_s[layer], xn_ss[layer]), functools.partial(up_store, layer)))
        if active(1):
            stages.append((lambda: dot(pwin_s[...], zn_s[...]), in_store))
        if active(0):
            stages.append((turn_rows, pair_store))
        return stages

    def run(its):
        waiting = []
        for it in its:
            stages = trip(it)
            for first_half, second_half in stages:
                waiting.append(functools.partial(second_half, first_half()))
                if len(waiting) > SKEW:
                    waiting.pop(0)()
            while waiting and len(stages) < SKEW + 2:
                waiting.pop(0)()
            yield
        for rest in waiting:
            rest()

    loops = (total - depth) // UNROLL

    def trips(i, carry):
        weave((run([depth + i * UNROLL + j for j in range(UNROLL)]), 1))
        return carry

    def turned():
        for b in range(n_blocks):
            for src, dst in ((wqkvg_ref, wqkvg_ts), (wao_ref, wao_ts), (wup_ref, wup_ts), (wdown_ref, wdown_ts)):
                dst[b] = jnp.transpose(src[b])
                yield

    weave((prepare(), 1), (tables(), PACE), (turned(), 1))
    z_copies[0].wait()

    def start():
        yield from gates(0, 1)
        xs_s[...] = sig_ref[0] * x_ref[...]
        begin(0)
        yield
        y_own[...] = pack(0, 0)

    weave((start(), 1), (run(range(depth)), 1))
    y_s[0, me] = y_own[...]
    for k in range(1, n_steps):
        u_s[k, me] = u_own[k]
    pl.semaphore_wait(barrier, n_peers - 1)
    for copy in copies(y_s, 0, *y_set):
        copy.start()
    for k in range(1, n_steps):
        for copy in copies(u_s, k, *u_set):
            copy.start()
    z_copies[1].wait()
    lax.fori_loop(0, loops, trips, 0)
    weave((run(range(depth + loops * UNROLL, total + depth)), 1))

    def turn(b):
        for h in range(n_heads):
            for key0 in range(0, n_tok, LANES):
                bias_ts[b, key0:key0 + LANES, h * tok_rows:(h + 1) * tok_rows] = jnp.transpose(bias_s[b * n_heads + h, :, key0:key0 + LANES])

    head = lax.broadcasted_iota(jnp.int32, (c_token, 1), 0) // head_dim
    scale = head_dim ** -0.5 * LOG2E
    cores = 2
    n_chips = n_peers // cores
    chip_keys = cores * tok_rows
    my_chip = me // cores

    def others(d, chip):
        return [me + 1 - 2 * lax.rem(me, cores)] if d == 0 else [chip * cores + c for c in range(cores)]

    def block(k, b):
        r = k * n_blocks + b
        rebuilt = k > 0 and b == 0
        y = pack(k, b) if rebuilt else y_s[r, me]
        q = dot(wqkvg_ts[b, :c_token, :], y)
        g = sigmoid(dot(wqkvg_ts[b, 3 * c_token:, :], y))
        q_heads = jnp.concatenate([jnp.where(head == h, q, 0.0).astype(BF16) for h in range(n_heads)], axis=1)
        tops, sums = [], []
        pos = 0
        for group in GROUPS if r > 0 else (sum(GROUPS, ()),):
            chips = [lax.rem(my_chip + d, n_chips) for d in group]
            for d, chip in zip(group, chips):
                for src in others(d, chip):
                    if rebuilt:
                        wait_from(r_s, k, *r_set, src)
                    else:
                        wait_from(y_s, r, *y_set, src)
            if rebuilt:
                parts = []
                for chip in chips:
                    keys = pl.ds(pl.multiple_of(chip * chip_keys, chip_keys), chip_keys)
                    pos_r = jnp.concatenate([r_s[k, chip * cores + c] for c in range(cores)], axis=1)
                    lin = pos_r[0:1] * jnp.concatenate([win_s[0]] * cores, axis=1)
                    for d in range(1, n_dim):
                        lin = lin + pos_r[d:d + 1] * jnp.concatenate([win_s[d]] * cores, axis=1)
                    parts.append((mul_all[:, keys] * norm_cols(lin + ast_all[:, keys]) + add_all[:, keys]).astype(BF16))
                y_group = jnp.concatenate(parts, axis=1)
            else:
                y_group = jnp.concatenate([y_s[r, chip * cores + c] for chip in chips for c in range(cores)], axis=1)
            kv = dot(wqkvg_ts[b, c_token:3 * c_token, :], y_group).astype(BF16)
            vt_s[:, pos * chip_keys:(pos + len(group)) * chip_keys] = kv[c_token:]
            scores = dot_tn(kv[:c_token], q_heads)
            for i, chip in enumerate(chips):
                key0 = pl.multiple_of(chip * chip_keys, chip_keys)
                sc = scores[i * chip_keys:(i + 1) * chip_keys] * scale + bias_ts[b, pl.ds(key0, chip_keys), :]
                key_ok = lax.broadcasted_iota(jnp.int32, (chip_keys, 1), 0) + key0 < n_valid
                sc = jnp.where(key_ok, sc, MASK_VALUE * LOG2E)
                top = jnp.max(sc, axis=0, keepdims=True)
                e = jnp.exp2(sc - top)
                e_s[pos] = e
                tops.append(top)
                sums.append(jnp.sum(e, axis=0, keepdims=True))
                pos += 1
        best = functools.reduce(jnp.maximum, tops)
        scales = [jnp.exp2(top - best) for top in tops]
        inv = 1.0 / functools.reduce(jnp.add, [f * l for f, l in zip(scales, sums)])
        probs = jnp.concatenate([(e_s[i] * (scales[i] * inv)).astype(BF16) for i in range(pos)], axis=0)
        mix = []
        for h in range(0, n_heads, 2):
            pair = dot(vt_s[h * head_dim:(h + 2) * head_dim, :], probs[:, h * tok_rows:(h + 2) * tok_rows])
            mix += [pair[:head_dim, :tok_rows], pair[head_dim:, tok_rows:]]
        attn = dot(wao_ts[b], (g * jnp.concatenate(mix, axis=0)).astype(BF16))
        acts = acts_s[...] + gate_s[k, b, 2] * attn
        normed = (gate_s[k, b, 3] * norm_cols(acts) + gate_s[k, b, 4]).astype(BF16)
        h = dot(wup_ts[b], normed)
        half = h.shape[0] // 2
        act = (silu(h[:half]) * h[half:]).astype(BF16)
        acts_s[...] = acts + gate_s[k, b, 5] * dot(wdown_ts[b], act)
        for copy in copies(r_s, k, *r_set) if rebuilt else copies(y_s, r, *y_set):
            copy.wait_send()

    turn(0)
    r_s[...] = jnp.zeros(r_s.shape, F32)
    for k in range(n_steps):
        if k > 0:
            r_s[k, me, :n_dim] = begin(k)
            for copy in copies(r_s, k, *r_set):
                copy.start()
            for off in range(1, n_peers):
                wait_from(u_s, k, *u_set, lax.rem(me + off, n_peers))
            u_all = jnp.concatenate([u_s[k, src] for src in range(n_peers)], axis=1)
            ast_all[...] = dot_tn(wstok_ref[...], u_all)
            mul_all[...] = sigmoid(dot_tn(wcond_ref[0, :, :c_token], u_all))
            add_all[...] = dot_tn(wcond_ref[0, :, c_token:2 * c_token], u_all)
        block(k, 0)
        for b in range(1, n_blocks):
            r = k * n_blocks + b
            y_s[r, me] = pack(k, b)
            for copy in copies(y_s, r, *y_set):
                copy.start()
            if k == 0:
                turn(b)
                if b == 1 and n_steps > 1:
                    weave((gates(1, n_steps), 1))
            block(k, b)
        if k == 0:
            for later in range(1, n_steps):
                for copy in copies(u_s, later, *u_set):
                    copy.wait_send()
        xn, t, var = noisy(k)
        update = dot(wout_ref[...], norm_cols(acts_s[...]).astype(BF16))
        denoised = (SIGMA_DATA * SIGMA_DATA / var) * xn + (t * SIGMA_DATA / jnp.sqrt(var)) * update
        xs_s[...] = xn + STEP_SCALE * (sig_ref[k + 1] - t) * (xn - denoised) / t
    out_ref[...] = xs_s[...]


def solution(mesh):
    part_axes = ("sample", "tok")
    n_peers = mesh.shape["tok"]

    def local_run(s_trunk, s_inputs, z_trunk, x_noise, step_noise, sigmas, relpos_table, w_pair_in, w_z_up, w_z_down, w_pair_bias, w_single, fourier_w, fourier_b, w_fourier, w_s_up, w_s_down, w_in, w_s_tok, w_cond, gate_bias, w_qkvg, w_attn_out, w_up, w_down, w_out):
        tok_rows, n_tok, c_pair = z_trunk.shape
        n_steps, _, n_dim = step_noise.shape
        n_blocks, _, n_heads = w_pair_bias.shape
        n_layers, _, width = w_z_up.shape
        c_token = w_qkvg.shape[1]
        clip = (relpos_table.shape[0] - 1) // 2
        tile = c_pair * SUB
        n_var = 2 * clip // SUB + LANES // SUB + 2
        n_rounds = n_steps * n_blocks
        swap = lambda a: jnp.swapaxes(a, -1, -2)
        ops = [
            sigmas, swap(z_trunk), swap(relpos_table), swap(w_pair_in), w_z_up, swap(w_z_down), swap(w_pair_bias),
            s_trunk, s_inputs, swap(x_noise), swap(step_noise), w_single, fourier_w[None, :], fourier_b[None, :], w_fourier, w_s_up, w_s_down,
            w_in, w_s_tok, w_cond, gate_bias, w_qkvg, w_attn_out, w_up, w_down, swap(w_out),
        ]
        specs = [pl.BlockSpec(memory_space=pltpu.SMEM), pl.BlockSpec(memory_space=pl.ANY)] + [pl.BlockSpec(memory_space=pltpu.VMEM)] * (len(ops) - 2)
        out = pl.pallas_call(
            functools.partial(kernel, "tok", n_peers),
            in_specs=specs,
            out_specs=pl.BlockSpec(memory_space=pltpu.VMEM),
            out_shape=jax.ShapeDtypeStruct((n_dim, tok_rows), F32),
            scratch_shapes=[
                pltpu.VMEM((tok_rows, c_pair, n_tok), BF16),
                pltpu.VMEM((n_blocks * n_heads, tok_rows, n_tok), F32),
                pltpu.VMEM((tile, 2 * tile), BF16),
                pltpu.VMEM((n_layers, width * SUB, tile), BF16),
                pltpu.VMEM((n_layers, tile, width // 2 * SUB), BF16),
                pltpu.VMEM((n_blocks * n_heads * SUB, tile), BF16),
                pltpu.VMEM((tile, tile), BF16),
                pltpu.VMEM((n_var, tile, LANES), F32),
                pltpu.VMEM((n_var, SUB, LANES), F32),
                pltpu.VMEM((2 * tile, CHUNK), BF16),
                pltpu.VMEM((n_layers + 1, tile, CHUNK), BF16),
                pltpu.VMEM((n_layers, tile, CHUNK), F32),
                pltpu.VMEM((n_layers, tile, CHUNK), F32),
                pltpu.VMEM((n_layers, width // 2 * SUB, CHUNK), BF16),
                pltpu.VMEM((n_blocks, n_tok, n_heads * tok_rows), F32),
                pltpu.VMEM((n_blocks, 4 * c_token, c_token), BF16),
                pltpu.VMEM((n_blocks, c_token, c_token), BF16),
                pltpu.VMEM((n_blocks, w_up.shape[2], c_token), BF16),
                pltpu.VMEM((n_blocks, c_token, w_down.shape[1]), BF16),
                pltpu.VMEM((c_token, SUB), F32),
                pltpu.VMEM((n_dim, c_token, tok_rows), F32),
                pltpu.VMEM((n_peers // 2, 2 * tok_rows, n_heads * tok_rows), F32),
                pltpu.VMEM((c_token, n_tok), BF16),
                pltpu.VMEM((c_token, tok_rows), F32),
                pltpu.VMEM((c_token, SUB), F32),
                pltpu.VMEM((n_steps, c_token, tok_rows), F32),
                pltpu.VMEM((n_steps, n_blocks, 6, c_token, tok_rows), F32),
                pltpu.VMEM((c_token, tok_rows), F32),
                pltpu.VMEM((n_dim, tok_rows), F32),
                pltpu.VMEM((n_rounds, n_peers, c_token, tok_rows), BF16),
                pltpu.VMEM((c_token, tok_rows), BF16),
                pltpu.VMEM((n_steps, c_token, tok_rows), BF16),
                pltpu.VMEM((n_steps, n_peers, c_token, tok_rows), BF16),
                pltpu.VMEM((n_steps, n_peers, SUB, tok_rows), F32),
                pltpu.VMEM((c_token, n_tok), F32),
                pltpu.VMEM((c_token, n_tok), F32),
                pltpu.VMEM((c_token, n_tok), F32),
                pltpu.SemaphoreType.DMA((2,)),
                pltpu.SemaphoreType.DMA((n_rounds, n_peers)),
                pltpu.SemaphoreType.DMA((n_rounds, n_peers)),
                pltpu.SemaphoreType.DMA((n_steps, n_peers)),
                pltpu.SemaphoreType.DMA((n_steps, n_peers)),
                pltpu.SemaphoreType.DMA((n_steps, n_peers)),
                pltpu.SemaphoreType.DMA((n_steps, n_peers)),
            ],
            compiler_params=pltpu.CompilerParams(collective_id=0, has_side_effects=True, vmem_limit_bytes=60 * 1024 * 1024),
            name="sampler",
        )(*ops)
        return swap(out)

    in_specs = (P("tok", None), P("tok", None), P("tok", None, None), P(part_axes, None), P(None, part_axes, None)) + (P(),) * 21
    return jax.shard_map(local_run, mesh=mesh, in_specs=in_specs, out_specs=P(part_axes, None), check_vma=False)
```
